8 devices in a mesh: dp: 1 (over z), sp: 8 (over y, x, core).
Axes of the slice: x: 2, y: 2, z: 1, core: 2. Of those that a mesh axis runs over, the one named last changes fastest.
Arguments:
- x: bfloat16 [8, 1024, 256], P('dp', 'sp')
- w_in: bfloat16 [10, 3, 256, 512], replicated
- w_res: bfloat16 [10, 256, 256], replicated
- w_skip: bfloat16 [10, 256, 256], replicated
Outputs:
- output 1: float32 [8, 1024, 256], P('dp', 'sp')
- output 2: float32 [8, 1024, 256], P('dp', 'sp')
All inputs are finite; a program needn't handle non-finite values.
Results may differ from the reference program's by a relative error of at most 0.0046347.
Values are sent between devices in bfloat16 or wider.
A program may use at most 1 GiB of HBM per device.

```python
import jax
import jax.numpy as jnp

NUM_SEQS = 8
SEQ_LEN = 1024
CHANNELS = 256
SKIP_CH = 256
NUM_LAYERS = 10


def setup_inputs(seed: int = 0, part: int = 0) -> dict:
    root_key = jax.random.key(seed)
    key_x, key_in, key_res, key_skip = jax.random.split(root_key, 4)
    x = jax.random.normal(jax.random.fold_in(key_x, part), (NUM_SEQS, SEQ_LEN, CHANNELS), jnp.float32)
    w_in = jax.random.normal(key_in, (NUM_LAYERS, 3, CHANNELS, 2 * CHANNELS), jnp.float32) * (3 * CHANNELS) ** -0.5
    w_res = jax.random.normal(key_res, (NUM_LAYERS, CHANNELS, CHANNELS), jnp.float32) * (0.5 * CHANNELS ** -0.5)
    w_skip = jax.random.normal(key_skip, (NUM_LAYERS, CHANNELS, SKIP_CH), jnp.float32) * CHANNELS ** -0.5
    return {'x': x.astype(jnp.bfloat16), 'w_in': w_in.astype(jnp.bfloat16), 'w_res': w_res.astype(jnp.bfloat16), 'w_skip': w_skip.astype(jnp.bfloat16)}


def matmul_rows(operand, weight):
    flat = jnp.dot(operand.reshape(-1, operand.shape[-1]), weight, preferred_element_type=jnp.float32)
    return flat.reshape(operand.shape[:-1] + (weight.shape[-1],))


def reference(x, w_in, w_res, w_skip):
    seq_len = x.shape[1]
    n_chan = x.shape[2]
    residual = x.astype(jnp.float32)
    skip_sum = jnp.zeros(x.shape[:2] + (w_skip.shape[2],), jnp.float32)
    for layer in range(NUM_LAYERS):
        dilation = 2 ** layer
        cur_bf = residual.astype(jnp.bfloat16)
        left_tap = jnp.pad(cur_bf[:, :seq_len - dilation], ((0, 0), (dilation, 0), (0, 0)))
        right_tap = jnp.pad(cur_bf[:, dilation:], ((0, 0), (0, dilation), (0, 0)))
        pre_act = matmul_rows(left_tap, w_in[layer, 0]) + matmul_rows(cur_bf, w_in[layer, 1]) + matmul_rows(right_tap, w_in[layer, 2])
        gated = (jnp.tanh(pre_act[..., :n_chan]) * jax.nn.sigmoid(pre_act[..., n_chan:])).astype(jnp.bfloat16)
        residual = residual + matmul_rows(gated, w_res[layer])
        skip_sum = skip_sum + matmul_rows(gated, w_skip[layer])
    return residual, skip_sum
```

```python
import functools

import jax
import jax.numpy as jnp
from jax import lax
from jax.experimental import pallas as pl
from jax.experimental.pallas import tpu as pltpu
from jax.sharding import PartitionSpec as P

F32, BF16 = jnp.float32, jnp.bfloat16
MESH = pl.DeviceIdType.MESH
LAYERS = 10
LOCAL = 7
SEQ, BLOCK, CHIP, CHAN = 1024, 128, 256, 256
TILE = 512


def pad_rows(layer):
    return max(2 ** layer, 16)


def flip(index, q):
    out = index
    for bit in range(3):
        if q >> bit & 1:
            out = out + 2 ** bit - 2 ** (bit + 1) * lax.rem(lax.div(index, 2 ** bit), 2)
    return out


def taps(load, d, n):
    centre = load(0, n)
    if d < 16:
        wide = load(-16, n + 32)
        return jnp.concatenate([wide[16 - d:16 - d + n], centre, wide[16 + d:16 + d + n]], axis=1)
    return jnp.concatenate([load(-d, n), centre, load(d, n)], axis=1)


def gated(rows, weight):
    z = jnp.dot(rows, weight, preferred_element_type=F32)
    half = jnp.tanh(z[:, CHAN:] * 0.5)
    return (jnp.tanh(z[:, :CHAN]) * (0.5 + 0.5 * half)).astype(BF16)


def dot(a, b):
    return jnp.dot(a, b, preferred_element_type=F32)


def kernel(x_ref, win_hbm, wres_hbm, wskip_hbm, oh_ref, os_ref, *scratch):
    su = scratch[:LAYERS]
    hu = scratch[LAYERS:LAYERS + LOCAL]
    (win, wres, wskip, hseq, hh, hs, fin_h, fin_s, sa, aland,
     wsem, xsend, xrecv, xloc, psem, hsend, hrecv, asend, arecv, fsem, floc) = scratch[LAYERS + LOCAL:]

    me = lax.axis_index('sp')
    chip, core = lax.div(me, 2), lax.rem(me, 2)
    partner = flip(me, 1)

    def remote(src, dst, send, recv, device):
        return pltpu.make_async_remote_copy(src_ref=src, dst_ref=dst, send_sem=send, recv_sem=recv,
                                            device_id={'sp': device}, device_id_type=MESH)

    weights = []
    for k in range(LAYERS):
        row = [pltpu.make_async_copy(win_hbm.at[k], win.at[k], wsem.at[k, 0]),
               pltpu.make_async_copy(wres_hbm.at[k], wres.at[pl.ds(k * CHAN, CHAN)], wsem.at[k, 1]),
               pltpu.make_async_copy(wskip_hbm.at[k], wskip.at[pl.ds(k * CHAN, CHAN)], wsem.at[k, 2])]
        for copy in row:
            copy.start()
        weights.append(row)

    barrier = pltpu.get_barrier_semaphore()
    for q in range(1, 8):
        pl.semaphore_signal(barrier, inc=1, device_id={'sp': flip(me, q)}, device_id_type=MESH)
    own_rows = pl.ds(pl.multiple_of(16 + BLOCK * me, 16), BLOCK)
    half_rows = pl.ds(pl.multiple_of(16 + BLOCK * core, 16), BLOCK)
    local = [pltpu.make_async_copy(x_ref.at[chip, core], su[0].at[own_rows], xloc.at[0]),
             pltpu.make_async_copy(x_ref.at[:, core], hu[0].at[:, half_rows], xloc.at[1])]
    for copy in local:
        copy.start()
    for k in range(LAYERS):
        pad = pad_rows(k)
        su[k][:pad, :] = jnp.zeros((pad, CHAN), BF16)
        su[k][pad + SEQ:, :] = jnp.zeros((pad, CHAN), BF16)
    pl.semaphore_wait(barrier, 7)

    spread = []
    for q in (6, 7, 2, 4, 3, 5, 1):
        to = flip(me, q)
        copy = remote(x_ref.at[lax.div(to, 2), lax.rem(to, 2)], su[0].at[own_rows], xsend.at[q], xrecv.at[q], to)
        copy.start()
        spread.append(copy)
    mate = remote(x_ref.at[:, 1 - core], hu[0].at[:, half_rows], psem.at[0], psem.at[1], partner)
    mate.start()

    sends = []

    def send_edges(k):
        pad = pad_rows(k)
        for r in range(4):
            there = lax.rem(chip + r, 4)
            for side in range(2):
                src = su[k].at[pl.ds(pl.multiple_of(CHIP * there + side * (CHIP + pad), 16), pad)]
                dst = hu[k].at[chip, pl.ds(side * (CHIP + pad), pad)]
                if r == 0:
                    pltpu.make_async_copy(src, dst, hrecv.at[k, chip, side]).start()
                else:
                    copy = remote(src, dst, hsend.at[k, r, side], hrecv.at[k, chip, side], 2 * there + core)
                    copy.start()
                    sends.append(copy)

    def wait_edges(k):
        pad = pad_rows(k)
        for i in range(4):
            for side in range(2):
                dst = hu[k].at[i, pl.ds(side * (CHIP + pad), pad)]
                pltpu.make_async_copy(dst, dst, hrecv.at[k, i, side]).wait()

    def send_gated(k):
        for q in range(8):
            to = flip(me, q)
            src = sa.at[k - LOCAL, pl.ds(pl.multiple_of(BLOCK * to, BLOCK), BLOCK)]
            dst = aland.at[k - LOCAL, me]
            if q == 0:
                copy = pltpu.make_async_copy(src, dst, arecv.at[k - LOCAL, 0])
            else:
                copy = remote(src, dst, asend.at[k - LOCAL, q], arecv.at[k - LOCAL, q], to)
                sends.append(copy)
            copy.start()

    def wait_gated(k):
        for q in range(8):
            dst = aland.at[k - LOCAL, flip(me, q)]
            pltpu.make_async_copy(dst, dst, arecv.at[k - LOCAL, q]).wait()

    def seq_layer(k):
        d, pad = 2 ** k, pad_rows(k)
        weights[k][0].wait()
        weights[k][1].wait()
        for row in range(0, SEQ, TILE):
            here = pl.ds(row, TILE)
            a = gated(taps(lambda start, size: su[k][pl.ds(row + pad + start, size), :], d, TILE), win[k])
            if k >= LOCAL:
                sa[k - LOCAL, here, :] = a
            if k < LAYERS - 1:
                new = hseq[here, :] + dot(a, wres[pl.ds(k * CHAN, CHAN), :])
                if k < LAYERS - 2:
                    hseq[here, :] = new
                su[k + 1][pl.ds(row + pad_rows(k + 1), TILE), :] = new.astype(BF16)

    def home_layer(k):
        d, pad = 2 ** k, pad_rows(k)
        weights[k][2].wait()
        for i in range(0, 4, 2):
            rows = jnp.concatenate([taps(lambda start, size: hu[k][j, pl.ds(pad + start, size), :], d, CHIP) for j in (i, i + 1)], axis=0)
            a = gated(rows, win[k])
            res = dot(a, wres[pl.ds(k * CHAN, CHAN), :])
            skip = dot(a, wskip[pl.ds(k * CHAN, CHAN), :])
            for j in range(2):
                for half in range(2):
                    cut = slice(j * CHIP + half * BLOCK, j * CHIP + (half + 1) * BLOCK)
                    new = hh[half, i + j] + res[cut]
                    hh[half, i + j] = new
                    hs[half, i + j] = skip[cut] if k == 0 else hs[half, i + j] + skip[cut]
                    if k < LOCAL - 1:
                        hu[k + 1][i + j, pl.ds(pad_rows(k + 1) + half * BLOCK, BLOCK), :] = new.astype(BF16)

    for copy in local:
        copy.wait()
    mate.wait()
    for half in range(2):
        hh[half] = hu[0][:, pl.ds(16 + half * BLOCK, BLOCK), :].astype(F32)
    for copy in spread:
        copy.wait()
    send_edges(0)
    hseq[...] = su[0][pl.ds(16, SEQ), :].astype(F32)
    for k in range(LAYERS):
        seq_layer(k)
        if k + 1 < LOCAL:
            send_edges(k + 1)
        if k >= LOCAL:
            send_gated(k)
    for k in range(LOCAL):
        wait_edges(k)
        home_layer(k)
    moves = []
    for n, (src, dst) in enumerate(((hh, fin_h), (hs, fin_s))):
        move = remote(src.at[1 - core], dst.at[:, core], fsem.at[n, 0], fsem.at[n, 1], partner)
        keep = pltpu.make_async_copy(src.at[core], dst.at[:, core], floc.at[n])
        move.start()
        keep.start()
        moves += [move, keep]
    for k in range(LOCAL, LAYERS):
        weights[k][2].wait()
    for move in moves:
        move.wait()

    def finish(first, last, into_h, into_s):
        a = jnp.concatenate([aland[k - LOCAL].reshape(8 * BLOCK, CHAN) for k in range(first, last)], axis=1)
        span = pl.ds(first * CHAN, (last - first) * CHAN)
        shape = (4, 2, BLOCK, CHAN)
        into_h[...] = fin_h[...] + dot(a, wres[span, :]).reshape(shape)
        into_s[...] = fin_s[...] + dot(a, wskip[span, :]).reshape(shape)

    wait_gated(7)
    wait_gated(8)
    finish(7, 9, fin_h, fin_s)
    wait_gated(9)
    finish(9, 10, oh_ref, os_ref)
    for copy in sends:
        copy.wait_send()


def solution(mesh):
    act_spec = P('dp', 'sp', None)

    def local_stack(x, w_in, w_res, w_skip):
        vmem = lambda shape, dtype: pltpu.VMEM(shape, dtype)
        dma = lambda *shape: pltpu.SemaphoreType.DMA(shape)
        out = jax.ShapeDtypeStruct((4, 2, BLOCK, CHAN), F32)
        scratch = [vmem((SEQ + 2 * pad_rows(k), CHAN), BF16) for k in range(LAYERS)]
        scratch += [vmem((4, CHIP + 2 * pad_rows(k), CHAN), BF16) for k in range(LOCAL)]
        scratch += [vmem((LAYERS, 3 * CHAN, 2 * CHAN), BF16), vmem((LAYERS * CHAN, CHAN), BF16), vmem((LAYERS * CHAN, CHAN), BF16),
                    vmem((SEQ, CHAN), F32), vmem((2, 4, BLOCK, CHAN), F32), vmem((2, 4, BLOCK, CHAN), F32),
                    vmem((4, 2, BLOCK, CHAN), F32), vmem((4, 2, BLOCK, CHAN), F32),
                    vmem((LAYERS - LOCAL, SEQ, CHAN), BF16), vmem((LAYERS - LOCAL, 8, BLOCK, CHAN), BF16)]
        scratch += [dma(LAYERS, 3), dma(8), dma(8), dma(2), dma(2), dma(LOCAL, 4, 2), dma(LOCAL, 4, 2), dma(3, 8), dma(3, 8), dma(2, 2), dma(2)]
        h, s = pl.pallas_call(
            kernel,
            out_shape=(out, out),
            in_specs=[pl.BlockSpec(memory_space=pl.ANY)] * 4,
            out_specs=(pl.BlockSpec(memory_space=pltpu.VMEM),) * 2,
            scratch_shapes=scratch,
            compiler_params=pltpu.CompilerParams(collective_id=0, has_side_effects=True, vmem_limit_bytes=56 * 2 ** 20),
        )(x.reshape(4, 2, BLOCK, CHAN), w_in.reshape(LAYERS, 3 * CHAN, 2 * CHAN), w_res, w_skip)
        return h.reshape(x.shape), s.reshape(x.shape)

    return jax.shard_map(local_stack, mesh=mesh, in_specs=(act_spec, P(), P(), P()), out_specs=(act_spec, act_spec), check_vma=False)
```

```python
import functools

import jax
import jax.numpy as jnp
from jax import lax
from jax.experimental import pallas as pl
from jax.experimental.pallas import tpu as pltpu
from jax.sharding import PartitionSpec as P

F32, BF16 = jnp.float32, jnp.bfloat16
MESH = pl.DeviceIdType.MESH
LAYERS = 10
LOCAL = 8
SEQ, BLOCK, CHIP, CHAN = 1024, 128, 256, 256
TILE = 512
STEP = 2
VMEM_LIMIT = 57 * 2 ** 20


def pad_rows(layer):
    return max(2 ** layer, 16)


def flip(index, q):
    out = index
    for bit in range(3):
        if q >> bit & 1:
            out = out + 2 ** bit - 2 ** (bit + 1) * lax.rem(lax.div(index, 2 ** bit), 2)
    return out


def taps(load, d, n):
    centre = load(0, n)
    if d < 16:
        wide = load(-16, n + 32)
        return jnp.concatenate([wide[16 - d:16 - d + n], centre, wide[16 + d:16 + d + n]], axis=1)
    return jnp.concatenate([load(-d, n), centre, load(d, n)], axis=1)


def gated(rows, weight):
    z = jnp.dot(rows, weight, preferred_element_type=F32)
    half = jnp.tanh(z[:, CHAN:] * 0.5)
    return (jnp.tanh(z[:, :CHAN]) * (0.5 + 0.5 * half)).astype(BF16)


def dot(a, b):
    return jnp.dot(a, b, preferred_element_type=F32)


def kernel(x_ref, win_hbm, wres_hbm, wskip_hbm, oh_ref, os_ref, last_ref, *scratch):
    su = scratch[:LAYERS]
    hu = scratch[LAYERS:LAYERS + LOCAL]
    (win, wres, wskip, hseq, hh, hs, fin_h, fin_s, sa, aland,
     wsem, xsend, xrecv, xloc, psem, hsend, hrecv, asend, arecv, fsem, floc, osem) = scratch[LAYERS + LOCAL:]

    me = lax.axis_index('sp')
    chip, core = lax.div(me, 2), lax.rem(me, 2)
    partner = flip(me, 1)

    def remote(src, dst, send, recv, device):
        return pltpu.make_async_remote_copy(src_ref=src, dst_ref=dst, send_sem=send, recv_sem=recv,
                                            device_id={'sp': device}, device_id_type=MESH)

    weights = []
    for k in range(LAYERS):
        row = [pltpu.make_async_copy(win_hbm.at[k], win.at[k], wsem.at[k, 0]),
               pltpu.make_async_copy(wres_hbm.at[k], wres.at[pl.ds(k * CHAN, CHAN)], wsem.at[k, 1]),
               pltpu.make_async_copy(wskip_hbm.at[k], wskip.at[pl.ds(k * CHAN, CHAN)], wsem.at[k, 2])]
        for copy in row:
            copy.start()
        weights.append(row)

    barrier = pltpu.get_barrier_semaphore()
    for q in range(1, 8):
        pl.semaphore_signal(barrier, inc=1, device_id={'sp': flip(me, q)}, device_id_type=MESH)
    own_rows = pl.ds(pl.multiple_of(16 + BLOCK * me, 16), BLOCK)
    half_rows = pl.ds(pl.multiple_of(16 + BLOCK * core, 16), BLOCK)
    local = [pltpu.make_async_copy(x_ref.at[chip, core], su[0].at[own_rows], xloc.at[0]),
             pltpu.make_async_copy(x_ref.at[:, core], hu[0].at[:, half_rows], xloc.at[1])]
    for copy in local:
        copy.start()
    for k in range(LAYERS):
        pad = pad_rows(k)
        su[k][:pad, :] = jnp.zeros((pad, CHAN), BF16)
        su[k][pad + SEQ:, :] = jnp.zeros((pad, CHAN), BF16)
    pl.semaphore_wait(barrier, 7)

    spread = []
    for q in (6, 7, 2, 4, 3, 5, 1):
        to = flip(me, q)
        copy = remote(x_ref.at[lax.div(to, 2), lax.rem(to, 2)], su[0].at[own_rows], xsend.at[q], xrecv.at[q], to)
        copy.start()
        spread.append(copy)
    mate = remote(x_ref.at[:, 1 - core], hu[0].at[:, half_rows], psem.at[0], psem.at[1], partner)
    mate.start()

    sends = []

    def send_edges(k):
        pad = pad_rows(k)
        for r in range(4):
            there = lax.rem(chip + r, 4)
            for side in range(2):
                src = su[k].at[pl.ds(pl.multiple_of(CHIP * there + side * (CHIP + pad), 16), pad)]
                dst = hu[k].at[chip, pl.ds(side * (CHIP + pad), pad)]
                if r == 0:
                    pltpu.make_async_copy(src, dst, hrecv.at[k, chip, side]).start()
                else:
                    copy = remote(src, dst, hsend.at[k, r, side], hrecv.at[k, chip, side], 2 * there + core)
                    copy.start()
                    sends.append(copy)

    def wait_edges(k):
        pad = pad_rows(k)
        for i in range(4):
            for side in range(2):
                dst = hu[k].at[i, pl.ds(side * (CHIP + pad), pad)]
                pltpu.make_async_copy(dst, dst, hrecv.at[k, i, side]).wait()

    def landing(k):
        return last_ref if k == LAYERS - 1 else aland.at[k - LOCAL]

    def send_gated(k):
        for q in range(8):
            to = flip(me, q)
            src = sa.at[k - LOCAL, pl.ds(pl.multiple_of(BLOCK * to, BLOCK), BLOCK)]
            dst = landing(k).at[me]
            if q == 0:
                copy = pltpu.make_async_copy(src, dst, arecv.at[k - LOCAL, 0])
            else:
                copy = remote(src, dst, asend.at[k - LOCAL, q], arecv.at[k - LOCAL, q], to)
                sends.append(copy)
            copy.start()

    def wait_gated(k):
        for q in range(8):
            dst = landing(k).at[flip(me, q)]
            pltpu.make_async_copy(dst, dst, arecv.at[k - LOCAL, q]).wait()

    def seq_layer(k):
        d, pad = 2 ** k, pad_rows(k)
        weights[k][0].wait()
        weights[k][1].wait()
        for row in range(0, SEQ, TILE):
            here = pl.ds(row, TILE)
            a = gated(taps(lambda start, size: su[k][pl.ds(row + pad + start, size), :], d, TILE), win[k])
            if k >= LOCAL:
                sa[k - LOCAL, here, :] = a
            if k < LAYERS - 1:
                new = hseq[here, :] + dot(a, wres[pl.ds(k * CHAN, CHAN), :])
                if k < LAYERS - 2:
                    hseq[here, :] = new
                su[k + 1][pl.ds(row + pad_rows(k + 1), TILE), :] = new.astype(BF16)

    def home_layer(k):
        d, pad = 2 ** k, pad_rows(k)
        weights[k][2].wait()
        for i in range(0, 4, 2):
            rows = jnp.concatenate([taps(lambda start, size: hu[k][j, pl.ds(pad + start, size), :], d, CHIP) for j in (i, i + 1)], axis=0)
            a = gated(rows, win[k])
            res = dot(a, wres[pl.ds(k * CHAN, CHAN), :])
            skip = dot(a, wskip[pl.ds(k * CHAN, CHAN), :])
            for j in range(2):
                for half in range(2):
                    cut = slice(j * CHIP + half * BLOCK, j * CHIP + (half + 1) * BLOCK)
                    new = hh[half, i + j] + res[cut]
                    hh[half, i + j] = new
                    hs[half, i + j] = skip[cut] if k == 0 else hs[half, i + j] + skip[cut]
                    if k < LOCAL - 1:
                        hu[k + 1][i + j, pl.ds(pad_rows(k + 1) + half * BLOCK, BLOCK), :] = new.astype(BF16)

    for copy in local:
        copy.wait()
    mate.wait()
    for half in range(2):
        hh[half] = hu[0][:, pl.ds(16 + half * BLOCK, BLOCK), :].astype(F32)
    for copy in spread:
        copy.wait()
    send_edges(0)
    hseq[...] = su[0][pl.ds(16, SEQ), :].astype(F32)
    for k in range(LAYERS):
        seq_layer(k)
        if k + 1 < LOCAL:
            send_edges(k + 1)
        if k >= LOCAL:
            send_gated(k)
    for k in range(LOCAL):
        wait_edges(k)
        home_layer(k)
    moves = []
    for n, (src, dst) in enumerate(((hh, fin_h), (hs, fin_s))):
        move = remote(src.at[1 - core], dst.at[:, core], fsem.at[n, 0], fsem.at[n, 1], partner)
        keep = pltpu.make_async_copy(src.at[core], dst.at[:, core], floc.at[n])
        move.start()
        keep.start()
        moves += [move, keep]
    for k in range(LOCAL, LAYERS):
        weights[k][2].wait()
    for move in moves:
        move.wait()
    for k in range(LOCAL, LAYERS - 1):
        wait_gated(k)
        span = pl.ds(k * CHAN, CHAN)
        a = aland[k - LOCAL].reshape(8 * BLOCK, CHAN)
        fin_h[...] = fin_h[...] + dot(a, wres[span, :]).reshape(fin_h.shape)
        fin_s[...] = fin_s[...] + dot(a, wskip[span, :]).reshape(fin_s.shape)
    outs = [pltpu.make_async_copy(fin_h, oh_ref, osem.at[0]), pltpu.make_async_copy(fin_s, os_ref, osem.at[1])]
    for out in outs:
        out.start()
    wait_gated(LAYERS - 1)
    for out in outs:
        out.wait()
    for copy in sends:
        copy.wait_send()


def last_layer(a_ref, h_ref, s_ref, wres_ref, wskip_ref, oh_ref, os_ref):
    a = a_ref[...].reshape(-1, CHAN)
    oh_ref[...] = h_ref[...] + dot(a, wres_ref[0]).reshape(h_ref.shape)
    os_ref[...] = s_ref[...] + dot(a, wskip_ref[0]).reshape(s_ref.shape)


def solution(mesh):
    act_spec = P('dp', 'sp', None)

    def local_stack(x, w_in, w_res, w_skip):
        vmem = lambda shape, dtype: pltpu.VMEM(shape, dtype)
        dma = lambda *shape: pltpu.SemaphoreType.DMA(shape)
        out = jax.ShapeDtypeStruct((4, 2, BLOCK, CHAN), F32)
        scratch = [vmem((SEQ + 2 * pad_rows(k), CHAN), BF16) for k in range(LAYERS)]
        scratch += [vmem((4, CHIP + 2 * pad_rows(k), CHAN), BF16) for k in range(LOCAL)]
        scratch += [vmem((LAYERS, 3 * CHAN, 2 * CHAN), BF16), vmem((LAYERS * CHAN, CHAN), BF16), vmem((LAYERS * CHAN, CHAN), BF16),
                    vmem((SEQ, CHAN), F32), vmem((2, 4, BLOCK, CHAN), F32), vmem((2, 4, BLOCK, CHAN), F32),
                    vmem((4, 2, BLOCK, CHAN), F32), vmem((4, 2, BLOCK, CHAN), F32),
                    vmem((LAYERS - LOCAL, SEQ, CHAN), BF16), vmem((LAYERS - LOCAL - 1, 8, BLOCK, CHAN), BF16)]
        scratch += [dma(LAYERS, 3), dma(8), dma(8), dma(2), dma(2), dma(LOCAL, 4, 2), dma(LOCAL, 4, 2), dma(LAYERS - LOCAL, 8), dma(LAYERS - LOCAL, 8), dma(2, 2), dma(2), dma(2)]
        h, s, a = pl.pallas_call(
            kernel,
            out_shape=(out, out, jax.ShapeDtypeStruct((8, BLOCK, CHAN), BF16)),
            in_specs=[pl.BlockSpec(memory_space=pltpu.HBM)] * 4,
            out_specs=(pl.BlockSpec(memory_space=pl.ANY),) * 3,
            scratch_shapes=scratch,
            compiler_params=pltpu.CompilerParams(collective_id=0, has_side_effects=True, vmem_limit_bytes=VMEM_LIMIT),
        )(x.reshape(4, 2, BLOCK, CHAN), w_in.reshape(LAYERS, 3 * CHAN, 2 * CHAN), w_res, w_skip)
        rows = pl.BlockSpec((STEP, BLOCK, CHAN), lambda i: (i, 0, 0))
        weight = pl.BlockSpec((1, CHAN, CHAN), lambda i: (LAYERS - 1, 0, 0))
        return pl.pallas_call(
            last_layer,
            grid=(8 // STEP,),
            out_shape=(jax.ShapeDtypeStruct(x.shape, F32),) * 2,
            in_specs=[rows, rows, rows, weight, weight],
            out_specs=(rows, rows),
        )(a, h.reshape(x.shape), s.reshape(x.shape), w_res, w_skip)

    return jax.shard_map(local_stack, mesh=mesh, in_specs=(act_spec, P(), P(), P()), out_specs=(act_spec, act_spec), check_vma=False)
```

```python
import functools

import jax
import jax.numpy as jnp
from jax import lax
from jax.experimental import pallas as pl
from jax.experimental.pallas import tpu as pltpu
from jax.sharding import PartitionSpec as P

F32, BF16 = jnp.float32, jnp.bfloat16
MESH = pl.DeviceIdType.MESH
LAYERS = 10
LOCAL = 8
SEQ, BLOCK, CHIP, CHAN = 1024, 128, 256, 256
TILE = 512
STEP = 4
VMEM_LIMIT = 50 * 2 ** 20


def pad_rows(layer):
    return max(2 ** layer, 16)


def flip(index, q):
    out = index
    for bit in range(3):
        if q >> bit & 1:
            out = out + 2 ** bit - 2 ** (bit + 1) * lax.rem(lax.div(index, 2 ** bit), 2)
    return out


def taps(load, d, n):
    centre = load(0, n)
    if d < 16:
        wide = load(-16, n + 32)
        return jnp.concatenate([wide[16 - d:16 - d + n], centre, wide[16 + d:16 + d + n]], axis=1)
    return jnp.concatenate([load(-d, n), centre, load(d, n)], axis=1)


def gated(rows, weight):
    z = jnp.dot(rows, weight, preferred_element_type=F32)
    half = jnp.tanh(z[:, CHAN:] * 0.5)
    return (jnp.tanh(z[:, :CHAN]) * (0.5 + 0.5 * half)).astype(BF16)


def dot(a, b):
    return jnp.dot(a, b, preferred_element_type=F32)


def kernel(x_ref, win_hbm, wres_hbm, wskip_hbm, oh_ref, os_ref, last_ref, wlast_ref, *scratch):
    su = scratch[:LAYERS]
    hu = scratch[LAYERS:LAYERS + LOCAL]
    (win, wres, wskip, hseq, hh, hs, fin_h, fin_s, sa, aland,
     wsem, xsend, xrecv, xloc, psem, hsend, hrecv, asend, arecv, fsem, floc, osem) = scratch[LAYERS + LOCAL:]

    me = lax.axis_index('sp')
    chip, core = lax.div(me, 2), lax.rem(me, 2)
    partner = flip(me, 1)

    def remote(src, dst, send, recv, device):
        return pltpu.make_async_remote_copy(src_ref=src, dst_ref=dst, send_sem=send, recv_sem=recv,
                                            device_id={'sp': device}, device_id_type=MESH)

    weights = []
    for k in range(LAYERS):
        row = [pltpu.make_async_copy(win_hbm.at[k], win.at[k], wsem.at[k, 0]),
               pltpu.make_async_copy(wres_hbm.at[k], wres.at[pl.ds(k * CHAN, CHAN)], wsem.at[k, 1]),
               pltpu.make_async_copy(wskip_hbm.at[k], wskip.at[pl.ds(k * CHAN, CHAN)], wsem.at[k, 2])]
        for copy in row:
            copy.start()
        weights.append(row)

    barrier = pltpu.get_barrier_semaphore()
    for q in range(1, 8):
        pl.semaphore_signal(barrier, inc=1, device_id={'sp': flip(me, q)}, device_id_type=MESH)
    own_rows = pl.ds(pl.multiple_of(16 + BLOCK * me, 16), BLOCK)
    half_rows = pl.ds(pl.multiple_of(16 + BLOCK * core, 16), BLOCK)
    local = [pltpu.make_async_copy(x_ref.at[chip, core], su[0].at[own_rows], xloc.at[0]),
             pltpu.make_async_copy(x_ref.at[:, core], hu[0].at[:, half_rows], xloc.at[1])]
    for copy in local:
        copy.start()
    for k in range(LAYERS):
        pad = pad_rows(k)
        su[k][:pad, :] = jnp.zeros((pad, CHAN), BF16)
        su[k][pad + SEQ:, :] = jnp.zeros((pad, CHAN), BF16)
    pl.semaphore_wait(barrier, 7)

    spread = []
    for q in (6, 7, 2, 4, 3, 5, 1):
        to = flip(me, q)
        copy = remote(x_ref.at[lax.div(to, 2), lax.rem(to, 2)], su[0].at[own_rows], xsend.at[q], xrecv.at[q], to)
        copy.start()
        spread.append(copy)
    mate = remote(x_ref.at[:, 1 - core], hu[0].at[:, half_rows], psem.at[0], psem.at[1], partner)
    mate.start()

    sends = []

    def send_edges(k):
        pad = pad_rows(k)
        for r in range(4):
            there = lax.rem(chip + r, 4)
            for side in range(2):
                src = su[k].at[pl.ds(pl.multiple_of(CHIP * there + side * (CHIP + pad), 16), pad)]
                dst = hu[k].at[chip, pl.ds(side * (CHIP + pad), pad)]
                if r == 0:
                    pltpu.make_async_copy(src, dst, hrecv.at[k, chip, side]).start()
                else:
                    copy = remote(src, dst, hsend.at[k, r, side], hrecv.at[k, chip, side], 2 * there + core)
                    copy.start()
                    sends.append(copy)

    def wait_edges(k):
        pad = pad_rows(k)
        for i in range(4):
            for side in range(2):
                dst = hu[k].at[i, pl.ds(side * (CHIP + pad), pad)]
                pltpu.make_async_copy(dst, dst, hrecv.at[k, i, side]).wait()

    def landing(k):
        return last_ref if k == LAYERS - 1 else aland.at[k - LOCAL]

    def send_gated(k):
        for q in range(8):
            to = flip(me, q)
            src = sa.at[k - LOCAL, pl.ds(pl.multiple_of(BLOCK * to, BLOCK), BLOCK)]
            dst = landing(k).at[me]
            if q == 0:
                copy = pltpu.make_async_copy(src, dst, arecv.at[k - LOCAL, 0])
            else:
                copy = remote(src, dst, asend.at[k - LOCAL, q], arecv.at[k - LOCAL, q], to)
                sends.append(copy)
            copy.start()

    def wait_gated(k):
        for q in range(8):
            dst = landing(k).at[flip(me, q)]
            pltpu.make_async_copy(dst, dst, arecv.at[k - LOCAL, q]).wait()

    def seq_layer(k):
        d, pad = 2 ** k, pad_rows(k)
        weights[k][0].wait()
        weights[k][1].wait()
        for row in range(0, SEQ, TILE):
            here = pl.ds(row, TILE)
            a = gated(taps(lambda start, size: su[k][pl.ds(row + pad + start, size), :], d, TILE), win[k])
            if k >= LOCAL:
                sa[k - LOCAL, here, :] = a
            if k < LAYERS - 1:
                new = hseq[here, :] + dot(a, wres[pl.ds(k * CHAN, CHAN), :])
                if k < LAYERS - 2:
                    hseq[here, :] = new
                su[k + 1][pl.ds(row + pad_rows(k + 1), TILE), :] = new.astype(BF16)

    def home_layer(k):
        d, pad = 2 ** k, pad_rows(k)
        weights[k][2].wait()
        for i in range(0, 4, 2):
            rows = jnp.concatenate([taps(lambda start, size: hu[k][j, pl.ds(pad + start, size), :], d, CHIP) for j in (i, i + 1)], axis=0)
            a = gated(rows, win[k])
            res = dot(a, wres[pl.ds(k * CHAN, CHAN), :])
            skip = dot(a, wskip[pl.ds(k * CHAN, CHAN), :])
            for j in range(2):
                for half in range(2):
                    cut = slice(j * CHIP + half * BLOCK, j * CHIP + (half + 1) * BLOCK)
                    new = hh[half, i + j] + res[cut]
                    hh[half, i + j] = new
                    hs[half, i + j] = skip[cut] if k == 0 else hs[half, i + j] + skip[cut]
                    if k < LOCAL - 1:
                        hu[k + 1][i + j, pl.ds(pad_rows(k + 1) + half * BLOCK, BLOCK), :] = new.astype(BF16)

    for copy in local:
        copy.wait()
    mate.wait()
    for half in range(2):
        hh[half] = hu[0][:, pl.ds(16 + half * BLOCK, BLOCK), :].astype(F32)
    for copy in spread:
        copy.wait()
    send_edges(0)
    hseq[...] = su[0][pl.ds(16, SEQ), :].astype(F32)
    for k in range(LAYERS):
        seq_layer(k)
        if k + 1 < LOCAL:
            send_edges(k + 1)
        if k >= LOCAL:
            send_gated(k)
    for k in range(LOCAL):
        wait_edges(k)
        home_layer(k)
    moves = []
    for n, (src, dst) in enumerate(((hh, fin_h), (hs, fin_s))):
        move = remote(src.at[1 - core], dst.at[:, core], fsem.at[n, 0], fsem.at[n, 1], partner)
        keep = pltpu.make_async_copy(src.at[core], dst.at[:, core], floc.at[n])
        move.start()
        keep.start()
        moves += [move, keep]
    for k in range(LOCAL, LAYERS):
        weights[k][2].wait()
    for move in moves:
        move.wait()
    for k in range(LOCAL, LAYERS - 1):
        wait_gated(k)
        span = pl.ds(k * CHAN, CHAN)
        a = aland[k - LOCAL].reshape(8 * BLOCK, CHAN)
        fin_h[...] = fin_h[...] + dot(a, wres[span, :]).reshape(fin_h.shape)
        fin_s[...] = fin_s[...] + dot(a, wskip[span, :]).reshape(fin_s.shape)
    final = pl.ds((LAYERS - 1) * CHAN, CHAN)
    outs = [pltpu.make_async_copy(fin_h, oh_ref, osem.at[0]), pltpu.make_async_copy(fin_s, os_ref, osem.at[1]),
            pltpu.make_async_copy(wres.at[final], wlast_ref.at[0], osem.at[2]), pltpu.make_async_copy(wskip.at[final], wlast_ref.at[1], osem.at[3])]
    for out in outs:
        out.start()
    wait_gated(LAYERS - 1)
    for out in outs:
        out.wait()
    for copy in sends:
        copy.wait_send()


def last_layer(a_ref, h_ref, s_ref, w_ref, oh_ref, os_ref):
    here = pl.ds(pl.program_id(0) * STEP, STEP)
    a = a_ref[here].reshape(STEP * BLOCK, CHAN)
    oh_ref[...] = h_ref[here] + dot(a, w_ref[0]).reshape(oh_ref.shape)
    os_ref[...] = s_ref[here] + dot(a, w_ref[1]).reshape(os_ref.shape)


def solution(mesh):
    act_spec = P('dp', 'sp', None)

    def local_stack(x, w_in, w_res, w_skip):
        vmem = lambda shape, dtype: pltpu.VMEM(shape, dtype)
        dma = lambda *shape: pltpu.SemaphoreType.DMA(shape)
        out = jax.ShapeDtypeStruct((4, 2, BLOCK, CHAN), F32)
        scratch = [vmem((SEQ + 2 * pad_rows(k), CHAN), BF16) for k in range(LAYERS)]
        scratch += [vmem((4, CHIP + 2 * pad_rows(k), CHAN), BF16) for k in range(LOCAL)]
        scratch += [vmem((LAYERS, 3 * CHAN, 2 * CHAN), BF16), vmem((LAYERS * CHAN, CHAN), BF16), vmem((LAYERS * CHAN, CHAN), BF16),
                    vmem((SEQ, CHAN), F32), vmem((2, 4, BLOCK, CHAN), F32), vmem((2, 4, BLOCK, CHAN), F32),
                    vmem((4, 2, BLOCK, CHAN), F32), vmem((4, 2, BLOCK, CHAN), F32),
                    vmem((LAYERS - LOCAL, SEQ, CHAN), BF16), vmem((LAYERS - LOCAL - 1, 8, BLOCK, CHAN), BF16)]
        scratch += [dma(LAYERS, 3), dma(8), dma(8), dma(2), dma(2), dma(LOCAL, 4, 2), dma(LOCAL, 4, 2), dma(LAYERS - LOCAL, 8), dma(LAYERS - LOCAL, 8), dma(2, 2), dma(2), dma(4)]
        h, s, a, w = pl.pallas_call(
            kernel,
            out_shape=(out, out, jax.ShapeDtypeStruct((8, BLOCK, CHAN), BF16), jax.ShapeDtypeStruct((2, CHAN, CHAN), BF16)),
            in_specs=[pl.BlockSpec(memory_space=pltpu.HBM)] * 4,
            out_specs=(pl.BlockSpec(memory_space=pl.ANY),) * 4,
            scratch_shapes=scratch,
            compiler_params=pltpu.CompilerParams(collective_id=0, has_side_effects=True, vmem_limit_bytes=VMEM_LIMIT),
        )(x.reshape(4, 2, BLOCK, CHAN), w_in.reshape(LAYERS, 3 * CHAN, 2 * CHAN), w_res, w_skip)
        rows = pl.BlockSpec((STEP, BLOCK, CHAN), lambda i: (i, 0, 0))
        return pl.pallas_call(
            last_layer,
            grid=(8 // STEP,),
            out_shape=(jax.ShapeDtypeStruct(x.shape, F32),) * 2,
            in_specs=[pl.BlockSpec(memory_space=pltpu.VMEM)] * 4,
            out_specs=(rows, rows),
            compiler_params=pltpu.CompilerParams(vmem_limit_bytes=8 * 2 ** 20),
        )(a, h.reshape(x.shape), s.reshape(x.shape), w)

    return jax.shard_map(local_stack, mesh=mesh, in_specs=(act_spec, P(), P(), P()), out_specs=(act_spec, act_spec), check_vma=False)
```

```python
import functools

import jax
import jax.numpy as jnp
from jax import lax
from jax.experimental import pallas as pl
from jax.experimental.pallas import tpu as pltpu
from jax.sharding import PartitionSpec as P

F32, BF16 = jnp.float32, jnp.bfloat16
MESH = pl.DeviceIdType.MESH
LAYERS = 10
LOCAL = 8
SEQ, BLOCK, CHIP, CHAN = 1024, 128, 256, 256
TILE = 512
STEP = 4
VMEM_LIMIT = 50 * 2 ** 20


EDGE = 128
EXTRA = [128, 128, 128, 112, 96, 64, 0, 0]
MARGIN = [144, 144, 144, 128, 112, 96, 64, 128]


def pad_rows(layer):
    return EDGE if layer == 0 else max(2 ** layer, 16)


def flip(index, q):
    out = index
    for bit in range(3):
        if q >> bit & 1:
            out = out + 2 ** bit - 2 ** (bit + 1) * lax.rem(lax.div(index, 2 ** bit), 2)
    return out


def taps(load, d, n):
    centre = load(0, n)
    if d < 16:
        wide = load(-16, n + 32)
        return jnp.concatenate([wide[16 - d:16 - d + n], centre, wide[16 + d:16 + d + n]], axis=1)
    return jnp.concatenate([load(-d, n), centre, load(d, n)], axis=1)


def gated(z):
    half = jnp.tanh(z[:, CHAN:] * 0.5)
    return (jnp.tanh(z[:, :CHAN]) * (0.5 + 0.5 * half)).astype(BF16)


def dot(a, b):
    return jnp.dot(a, b, preferred_element_type=F32)


def kernel(x_ref, win_hbm, wres_hbm, wskip_hbm, oh_ref, os_ref, last_ref, wlast_ref, *scratch):
    su = scratch[:LAYERS]
    hu = scratch[LAYERS:LAYERS + LOCAL]
    (win, wres, wskip, hseq, hh, hs, own_s, fin_h, fin_s, sa, aland,
     wsem, xsend, xrecv, xloc, psend, precv, hsend, hrecv, asend, arecv, fsend, frecv, floc, osem) = scratch[LAYERS + LOCAL:]

    me = lax.axis_index('sp')
    chip, core = lax.div(me, 2), lax.rem(me, 2)
    partner = flip(me, 1)
    pair = [chip] + [lax.rem(chip + r, 4) for r in (1, 2, 3)]

    def remote(src, dst, send, recv, device):
        return pltpu.make_async_remote_copy(src_ref=src, dst_ref=dst, send_sem=send, recv_sem=recv,
                                            device_id={'sp': device}, device_id_type=MESH)

    def block(start):
        return pl.ds(pl.multiple_of(start, 16), BLOCK)

    weights = []
    for k in range(LAYERS):
        row = [pltpu.make_async_copy(win_hbm.at[k], win.at[k], wsem.at[k, 0]),
               pltpu.make_async_copy(wres_hbm.at[k], wres.at[pl.ds(k * CHAN, CHAN)], wsem.at[k, 1]),
               pltpu.make_async_copy(wskip_hbm.at[k], wskip.at[pl.ds(k * CHAN, CHAN)], wsem.at[k, 2])]
        for copy in row:
            copy.start()
        weights.append(row)

    barrier = pltpu.get_barrier_semaphore()
    for q in range(1, 8):
        pl.semaphore_signal(barrier, inc=1, device_id={'sp': flip(me, q)}, device_id_type=MESH)
    own_rows = block(EDGE + BLOCK * me)
    half_rows = block(MARGIN[0] + BLOCK * core)
    local = [pltpu.make_async_copy(x_ref.at[chip, core], su[0].at[own_rows], xloc.at[0])]
    local += [pltpu.make_async_copy(x_ref.at[pair[r], core], hu[0].at[r - 1, half_rows], xloc.at[r]) for r in (1, 2, 3)]
    for copy in local:
        copy.start()
    for k in range(LAYERS):
        pad = pad_rows(k)
        su[k][:pad, :] = jnp.zeros((pad, CHAN), BF16)
        su[k][pad + SEQ:, :] = jnp.zeros((pad, CHAN), BF16)
    for k in range(3):
        for r in range(3):
            hu[k][r, :16, :] = jnp.zeros((16, CHAN), BF16)
            hu[k][r, CHIP + 2 * MARGIN[k] - 16:, :] = jnp.zeros((16, CHAN), BF16)
    pl.semaphore_wait(barrier, 7)

    spread = []
    for q in (6, 7, 2, 4, 3, 5, 1):
        to = flip(me, q)
        copy = remote(x_ref.at[lax.div(to, 2), lax.rem(to, 2)], su[0].at[own_rows], xsend.at[q], xrecv.at[q], to)
        copy.start()
        spread.append(copy)
    mates = [remote(x_ref.at[pair[r], 1 - core], hu[0].at[r - 1, half_rows], psend.at[r], precv.at[r], partner) for r in (1, 2, 3)]
    for copy in mates:
        copy.start()

    sends = []

    def send_edges(k, n):
        for r in (1, 2, 3):
            for side in range(2):
                src = su[k].at[block(CHIP * pair[r] + side * (CHIP + EDGE))]
                dst = hu[k].at[3 - r, pl.ds(MARGIN[k] - EDGE + side * (CHIP + EDGE), EDGE)]
                copy = remote(src, dst, hsend.at[n, r, side], hrecv.at[n, 3 - r, side], 2 * pair[r] + core)
                copy.start()
                sends.append(copy)

    def wait_edges(k, n):
        for r in range(3):
            for side in range(2):
                dst = hu[k].at[r, pl.ds(MARGIN[k] - EDGE + side * (CHIP + EDGE), EDGE)]
                pltpu.make_async_copy(dst, dst, hrecv.at[n, r, side]).wait()

    def landing(k):
        return last_ref if k == LAYERS - 1 else aland.at[k - LOCAL]

    def send_gated(k):
        for q in range(8):
            to = flip(me, q)
            src = sa.at[k, block(BLOCK * to)]
            dst = landing(k).at[me]
            if q == 0:
                copy = pltpu.make_async_copy(src, dst, arecv.at[k - LOCAL, 0])
            else:
                copy = remote(src, dst, asend.at[k - LOCAL, q], arecv.at[k - LOCAL, q], to)
                sends.append(copy)
            copy.start()

    def wait_gated(k):
        for q in range(8):
            dst = landing(k).at[flip(me, q)]
            pltpu.make_async_copy(dst, dst, arecv.at[k - LOCAL, q]).wait()

    def seq_layer(k):
        d, pad = 2 ** k, pad_rows(k)
        weights[k][0].wait()
        weights[k][1].wait()
        rows = range(0, SEQ, TILE)
        pre = [dot(taps(lambda start, size: su[k][pl.ds(row + pad + start, size), :], d, TILE), win[k]) for row in rows]
        for row, z in zip(rows, pre):
            here = pl.ds(row, TILE)
            a = gated(z)
            sa[k, here, :] = a
            if k < LAYERS - 1:
                new = hseq[here, :] + dot(a, wres[pl.ds(k * CHAN, CHAN), :])
                if k < LOCAL:
                    hseq[here, :] = new
                su[k + 1][pl.ds(row + pad_rows(k + 1), TILE), :] = new.astype(BF16)

    def home_layer(k):
        d, extra, margin = 2 ** k, EXTRA[k], MARGIN[k]
        size = CHIP + 2 * extra
        here = pl.ds(EDGE - extra, size)
        weights[k][2].wait()
        pre = [dot(taps(lambda start, n: hu[k][r, pl.ds(margin - extra + start, n), :], d, size), win[k]) for r in range(3)]
        for r, z in enumerate(pre):
            a = gated(z)
            new = hh[r, here, :] + dot(a, wres[pl.ds(k * CHAN, CHAN), :])
            hh[r, here, :] = new
            skip = dot(a[extra:extra + CHIP], wskip[pl.ds(k * CHAN, CHAN), :])
            hs[r] = skip if k == 0 else hs[r] + skip
            if k < LOCAL - 1:
                base = MARGIN[k + 1]
                hu[k + 1][r, pl.ds(base, CHIP), :] = new[extra:extra + CHIP].astype(BF16)
                if extra:
                    hu[k + 1][r, pl.ds(base - extra, extra), :] = jnp.where(chip > 0, new[:extra], 0.0).astype(BF16)
                    hu[k + 1][r, pl.ds(base + CHIP, extra), :] = jnp.where(chip < 3, new[extra + CHIP:], 0.0).astype(BF16)

    local[0].wait()
    for copy in spread:
        copy.wait()
    send_edges(0, 0)
    hseq[...] = su[0][pl.ds(EDGE, SEQ), :].astype(F32)
    for k in range(LAYERS):
        seq_layer(k)
        if k == LOCAL - 2:
            send_edges(LOCAL - 1, 1)
        if k >= LOCAL:
            send_gated(k)
    for copy in local[1:] + mates:
        copy.wait()
    wait_edges(0, 0)
    for r in range(3):
        hh[r] = hu[0][r, pl.ds(MARGIN[0] - EDGE, CHIP + 2 * EDGE), :].astype(F32)
    for k in range(LOCAL):
        if k == LOCAL - 1:
            wait_edges(k, 1)
        home_layer(k)
    mine = pl.ds(pl.multiple_of(CHIP * chip, CHIP), CHIP)
    own_s[...] = dot(jnp.concatenate([sa[k, mine, :] for k in range(LOCAL)], axis=1), wskip[pl.ds(0, LOCAL * CHAN), :])
    moves = []
    for r in range(4):
        for n, dst in enumerate((fin_h, fin_s)):
            def half(which):
                if r:
                    return (hh.at[r - 1, block(EDGE + BLOCK * which)], hs.at[r - 1, block(BLOCK * which)])[n]
                return (hseq.at[block(CHIP * chip + BLOCK * which)], own_s.at[block(BLOCK * which)])[n]
            moves += [remote(half(1 - core), dst.at[pair[r], core], fsend.at[r, n], frecv.at[r, n], partner),
                      pltpu.make_async_copy(half(core), dst.at[pair[r], core], floc.at[r, n])]
    for move in moves:
        move.start()
    for k in range(LOCAL, LAYERS):
        weights[k][2].wait()
    for move in moves:
        move.wait()
    for k in range(LOCAL, LAYERS - 1):
        wait_gated(k)
        span = pl.ds(k * CHAN, CHAN)
        a = aland[k - LOCAL].reshape(8 * BLOCK, CHAN)
        fin_h[...] = fin_h[...] + dot(a, wres[span, :]).reshape(fin_h.shape)
        fin_s[...] = fin_s[...] + dot(a, wskip[span, :]).reshape(fin_s.shape)
    final = pl.ds((LAYERS - 1) * CHAN, CHAN)
    outs = [pltpu.make_async_copy(fin_h, oh_ref, osem.at[0]), pltpu.make_async_copy(fin_s, os_ref, osem.at[1]),
            pltpu.make_async_copy(wres.at[final], wlast_ref.at[0], osem.at[2]), pltpu.make_async_copy(wskip.at[final], wlast_ref.at[1], osem.at[3])]
    for out in outs:
        out.start()
    wait_gated(LAYERS - 1)
    for out in outs:
        out.wait()
    for copy in sends:
        copy.wait_send()


def last_layer(a_ref, h_ref, s_ref, w_ref, oh_ref, os_ref):
    here = pl.ds(pl.program_id(0) * STEP, STEP)
    a = a_ref[here].reshape(STEP * BLOCK, CHAN)
    oh_ref[...] = h_ref[here] + dot(a, w_ref[0]).reshape(oh_ref.shape)
    os_ref[...] = s_ref[here] + dot(a, w_ref[1]).reshape(os_ref.shape)


def solution(mesh):
    act_spec = P('dp', 'sp', None)

    def local_stack(x, w_in, w_res, w_skip):
        vmem = lambda shape, dtype: pltpu.VMEM(shape, dtype)
        dma = lambda *shape: pltpu.SemaphoreType.DMA(shape)
        out = jax.ShapeDtypeStruct((4, 2, BLOCK, CHAN), F32)
        scratch = [vmem((SEQ + 2 * pad_rows(k), CHAN), BF16) for k in range(LAYERS)]
        scratch += [vmem((3, CHIP + 2 * MARGIN[k], CHAN), BF16) for k in range(LOCAL)]
        scratch += [vmem((LAYERS, 3 * CHAN, 2 * CHAN), BF16), vmem((LAYERS * CHAN, CHAN), BF16), vmem((LAYERS * CHAN, CHAN), BF16),
                    vmem((SEQ, CHAN), F32), vmem((3, CHIP + 2 * EDGE, CHAN), F32), vmem((3, CHIP, CHAN), F32), vmem((CHIP, CHAN), F32),
                    vmem((4, 2, BLOCK, CHAN), F32), vmem((4, 2, BLOCK, CHAN), F32),
                    vmem((LAYERS, SEQ, CHAN), BF16), vmem((LAYERS - LOCAL - 1, 8, BLOCK, CHAN), BF16)]
        scratch += [dma(LAYERS, 3), dma(8), dma(8), dma(4), dma(4), dma(4), dma(2, 4, 2), dma(2, 3, 2),
                    dma(LAYERS - LOCAL, 8), dma(LAYERS - LOCAL, 8), dma(4, 2), dma(4, 2), dma(4, 2), dma(4)]
        h, s, a, w = pl.pallas_call(
            kernel,
            out_shape=(out, out, jax.ShapeDtypeStruct((8, BLOCK, CHAN), BF16), jax.ShapeDtypeStruct((2, CHAN, CHAN), BF16)),
            in_specs=[pl.BlockSpec(memory_space=pltpu.HBM)] * 4,
            out_specs=(pl.BlockSpec(memory_space=pl.ANY),) * 4,
            scratch_shapes=scratch,
            compiler_params=pltpu.CompilerParams(collective_id=0, has_side_effects=True, vmem_limit_bytes=VMEM_LIMIT),
        )(pltpu.with_memory_space_constraint(x.reshape(4, 2, BLOCK, CHAN), pltpu.HBM), w_in.reshape(LAYERS, 3 * CHAN, 2 * CHAN), w_res, w_skip)
        rows = pl.BlockSpec((STEP, BLOCK, CHAN), lambda i: (i, 0, 0))
        return pl.pallas_call(
            last_layer,
            grid=(8 // STEP,),
            out_shape=(jax.ShapeDtypeStruct(x.shape, F32),) * 2,
            in_specs=[pl.BlockSpec(memory_space=pltpu.VMEM)] * 4,
            out_specs=(rows, rows),
            compiler_params=pltpu.CompilerParams(vmem_limit_bytes=8 * 2 ** 20),
        )(a, h.reshape(x.shape), s.reshape(x.shape), w)

    return jax.shard_map(local_stack, mesh=mesh, in_specs=(act_spec, P(), P(), P()), out_specs=(act_spec, act_spec), check_vma=False)
```

```python
import functools

import jax
import jax.numpy as jnp
from jax import lax
from jax.experimental import pallas as pl
from jax.experimental.pallas import tpu as pltpu
from jax.sharding import PartitionSpec as P

F32, BF16 = jnp.float32, jnp.bfloat16
MESH = pl.DeviceIdType.MESH
LAYERS = 10
LOCAL = 8
SEQ, BLOCK, CHIP, CHAN = 1024, 128, 256, 256
TILE = 512
EARLY = 3
STEP = 4
VMEM_LIMIT = 50 * 2 ** 20


EDGE = 128
EXTRA = [128, 128, 128, 112, 96, 64, 0, 0]
MARGIN = [144, 144, 144, 128, 112, 96, 64, 128]


def pad_rows(layer):
    return EDGE if layer == 0 else max(2 ** layer, 16)


def flip(index, q):
    out = index
    for bit in range(3):
        if q >> bit & 1:
            out = out + 2 ** bit - 2 ** (bit + 1) * lax.rem(lax.div(index, 2 ** bit), 2)
    return out


def taps(load, d, n):
    centre = load(0, n)
    if d < 16:
        wide = load(-16, n + 32)
        return jnp.concatenate([wide[16 - d:16 - d + n], centre, wide[16 + d:16 + d + n]], axis=1)
    return jnp.concatenate([load(-d, n), centre, load(d, n)], axis=1)


def gated(z):
    half = jnp.tanh(z[:, CHAN:] * 0.5)
    return (jnp.tanh(z[:, :CHAN]) * (0.5 + 0.5 * half)).astype(BF16)


def dot(a, b):
    return jnp.dot(a, b, preferred_element_type=F32)


def kernel(x_ref, win_hbm, wres_hbm, wskip_hbm, oh_ref, os_ref, last_ref, wlast_ref, *scratch):
    su = scratch[:LAYERS]
    hu = scratch[LAYERS:LAYERS + LOCAL]
    (win, wres, wskip, hseq, hh, hs, own_s, fin_h, fin_s, sa, aland,
     wsem, xsend, xrecv, xloc, psend, precv, hsend, hrecv, asend, arecv, fsend, frecv, floc, osem, relay) = scratch[LAYERS + LOCAL:]

    me = lax.axis_index('sp')
    chip, core = lax.div(me, 2), lax.rem(me, 2)
    partner = flip(me, 1)
    pair = [chip] + [lax.rem(chip + r, 4) for r in (1, 2, 3)]

    def remote(src, dst, send, recv, device):
        return pltpu.make_async_remote_copy(src_ref=src, dst_ref=dst, send_sem=send, recv_sem=recv,
                                            device_id={'sp': device}, device_id_type=MESH)

    def block(start):
        return pl.ds(pl.multiple_of(start, 16), BLOCK)

    weights = []
    for k in range(LAYERS):
        row = [pltpu.make_async_copy(win_hbm.at[k], win.at[k], wsem.at[k, 0]),
               pltpu.make_async_copy(wres_hbm.at[k], wres.at[pl.ds(k * CHAN, CHAN)], wsem.at[k, 1]),
               pltpu.make_async_copy(wskip_hbm.at[k], wskip.at[pl.ds(k * CHAN, CHAN)], wsem.at[k, 2])]
        for copy in row:
            copy.start()
        weights.append(row)

    barrier = pltpu.get_barrier_semaphore()
    for q in range(1, 6):
        pl.semaphore_signal(barrier, inc=1, device_id={'sp': flip(me, q)}, device_id_type=MESH)
    own_rows = block(EDGE + BLOCK * me)
    half_rows = block(MARGIN[0] + BLOCK * core)
    local = [pltpu.make_async_copy(x_ref.at[chip, core], su[0].at[own_rows], xloc.at[0])]
    local += [pltpu.make_async_copy(x_ref.at[pair[r], core], hu[0].at[r - 1, half_rows], xloc.at[r]) for r in (1, 2, 3)]
    for copy in local:
        copy.start()
    for k in range(LAYERS):
        pad = pad_rows(k)
        su[k][:pad, :] = jnp.zeros((pad, CHAN), BF16)
        su[k][pad + SEQ:, :] = jnp.zeros((pad, CHAN), BF16)
    for k in range(3):
        for r in range(3):
            hu[k][r, :16, :] = jnp.zeros((16, CHAN), BF16)
            hu[k][r, CHIP + 2 * MARGIN[k] - 16:, :] = jnp.zeros((16, CHAN), BF16)
    pl.semaphore_wait(barrier, 5)
    pl.semaphore_signal(relay, inc=1, device_id={'sp': flip(me, 2)}, device_id_type=MESH)

    spread = {}
    for q in (2, 4, 3, 5, 1, 6, 7):
        if q == 6:
            pl.semaphore_wait(relay, 1)
        to = flip(me, q)
        spread[q] = remote(x_ref.at[lax.div(to, 2), lax.rem(to, 2)], su[0].at[own_rows], xsend.at[q], xrecv.at[q], to)
        spread[q].start()
    mates = [remote(x_ref.at[pair[r], 1 - core], hu[0].at[r - 1, half_rows], psend.at[r], precv.at[r], partner) for r in (1, 2, 3)]
    for copy in mates:
        copy.start()

    sends = []

    def send_edges(k, n):
        for r in (1, 2, 3):
            for side in range(2):
                src = su[k].at[block(CHIP * pair[r] + side * (CHIP + EDGE))]
                dst = hu[k].at[3 - r, pl.ds(MARGIN[k] - EDGE + side * (CHIP + EDGE), EDGE)]
                copy = remote(src, dst, hsend.at[n, r, side], hrecv.at[n, 3 - r, side], 2 * pair[r] + core)
                copy.start()
                sends.append(copy)

    def wait_edges(k, n):
        for r in range(3):
            for side in range(2):
                dst = hu[k].at[r, pl.ds(MARGIN[k] - EDGE + side * (CHIP + EDGE), EDGE)]
                pltpu.make_async_copy(dst, dst, hrecv.at[n, r, side]).wait()

    def landing(k):
        return last_ref if k == LAYERS - 1 else aland.at[k - LOCAL]

    def send_gated(k):
        for q in range(8):
            to = flip(me, q)
            src = sa.at[k, block(BLOCK * to)]
            dst = landing(k).at[me]
            if q == 0:
                copy = pltpu.make_async_copy(src, dst, arecv.at[k - LOCAL, 0])
            else:
                copy = remote(src, dst, asend.at[k - LOCAL, q], arecv.at[k - LOCAL, q], to)
                sends.append(copy)
            copy.start()

    def wait_gated(k):
        for q in range(8):
            dst = landing(k).at[flip(me, q)]
            pltpu.make_async_copy(dst, dst, arecv.at[k - LOCAL, q]).wait()

    def seq_layer(k, tiles):
        d, pad = 2 ** k, pad_rows(k)

        def rows_at(start, size):
            return pl.ds(start if isinstance(start, int) else pl.multiple_of(start, 16), size)

        pre = [dot(taps(lambda start, n: su[k][rows_at(row + pad + start, n), :], d, size), win[k]) for row, size in tiles]
        for (row, size), z in zip(tiles, pre):
            here = rows_at(row, size)
            a = gated(z)
            sa[k, here, :] = a
            if k < LAYERS - 1:
                new = hseq[here, :] + dot(a, wres[pl.ds(k * CHAN, CHAN), :])
                if k < LOCAL:
                    hseq[here, :] = new
                su[k + 1][rows_at(row + pad_rows(k + 1), size), :] = new.astype(BF16)

    def home_layer(k):
        d, extra, margin = 2 ** k, EXTRA[k], MARGIN[k]
        size = CHIP + 2 * extra
        here = pl.ds(EDGE - extra, size)
        weights[k][2].wait()
        pre = [dot(taps(lambda start, n: hu[k][r, pl.ds(margin - extra + start, n), :], d, size), win[k]) for r in range(3)]
        for r, z in enumerate(pre):
            a = gated(z)
            new = hh[r, here, :] + dot(a, wres[pl.ds(k * CHAN, CHAN), :])
            hh[r, here, :] = new
            skip = dot(a[extra:extra + CHIP], wskip[pl.ds(k * CHAN, CHAN), :])
            hs[r] = skip if k == 0 else hs[r] + skip
            if k < LOCAL - 1:
                base = MARGIN[k + 1]
                hu[k + 1][r, pl.ds(base, CHIP), :] = new[extra:extra + CHIP].astype(BF16)
                if extra:
                    hu[k + 1][r, pl.ds(base - extra, extra), :] = jnp.where(chip > 0, new[:extra], 0.0).astype(BF16)
                    hu[k + 1][r, pl.ds(base + CHIP, extra), :] = jnp.where(chip < 3, new[extra + CHIP:], 0.0).astype(BF16)

    low = lax.div(chip, 2)
    local[0].wait()
    for q in (1, 2, 3):
        spread[q].wait()
    near, far = (pl.multiple_of(which * TILE, 16) for which in (low, 1 - low))
    hseq[pl.ds(near, TILE), :] = su[0][pl.ds(pl.multiple_of(EDGE + near, 16), TILE), :].astype(F32)
    for k in range(EARLY):
        weights[k][0].wait()
        weights[k][1].wait()
        size = TILE - 16 * (k + 1)
        seq_layer(k, [(low * (SEQ - size), size)])
    for q in (4, 5, 6, 7):
        spread[q].wait()
    send_edges(0, 0)
    hseq[pl.ds(far, TILE), :] = su[0][pl.ds(pl.multiple_of(EDGE + far, 16), TILE), :].astype(F32)
    for k in range(LAYERS):
        if k < EARLY:
            size = TILE + 16 * (k + 1)
            start, part = (1 - low) * (SEQ - size), 16 * (size // 32)
            seq_layer(k, [(start, part), (start + part, size - part)])
        else:
            weights[k][0].wait()
            weights[k][1].wait()
            seq_layer(k, [(row, TILE) for row in range(0, SEQ, TILE)])
        if k == LOCAL - 2:
            send_edges(LOCAL - 1, 1)
        if k >= LOCAL:
            send_gated(k)
    for copy in local[1:] + mates:
        copy.wait()
    wait_edges(0, 0)
    for r in range(3):
        hh[r] = hu[0][r, pl.ds(MARGIN[0] - EDGE, CHIP + 2 * EDGE), :].astype(F32)
    for k in range(LOCAL):
        if k == LOCAL - 1:
            wait_edges(k, 1)
        home_layer(k)
    mine = pl.ds(pl.multiple_of(CHIP * chip, CHIP), CHIP)
    own_s[...] = dot(jnp.concatenate([sa[k, mine, :] for k in range(LOCAL)], axis=1), wskip[pl.ds(0, LOCAL * CHAN), :])
    moves = []
    for r in range(4):
        for n, dst in enumerate((fin_h, fin_s)):
            def half(which):
                if r:
                    return (hh.at[r - 1, block(EDGE + BLOCK * which)], hs.at[r - 1, block(BLOCK * which)])[n]
                return (hseq.at[block(CHIP * chip + BLOCK * which)], own_s.at[block(BLOCK * which)])[n]
            moves += [remote(half(1 - core), dst.at[pair[r], core], fsend.at[r, n], frecv.at[r, n], partner),
                      pltpu.make_async_copy(half(core), dst.at[pair[r], core], floc.at[r, n])]
    for move in moves:
        move.start()
    for k in range(LOCAL, LAYERS):
        weights[k][2].wait()
    for move in moves:
        move.wait()
    for k in range(LOCAL, LAYERS - 1):
        wait_gated(k)
        span = pl.ds(k * CHAN, CHAN)
        a = aland[k - LOCAL].reshape(8 * BLOCK, CHAN)
        fin_h[...] = fin_h[...] + dot(a, wres[span, :]).reshape(fin_h.shape)
        fin_s[...] = fin_s[...] + dot(a, wskip[span, :]).reshape(fin_s.shape)
    final = pl.ds((LAYERS - 1) * CHAN, CHAN)
    outs = [pltpu.make_async_copy(fin_h, oh_ref, osem.at[0]), pltpu.make_async_copy(fin_s, os_ref, osem.at[1]),
            pltpu.make_async_copy(wres.at[final], wlast_ref.at[0], osem.at[2]), pltpu.make_async_copy(wskip.at[final], wlast_ref.at[1], osem.at[3])]
    for out in outs:
        out.start()
    wait_gated(LAYERS - 1)
    for out in outs:
        out.wait()
    for copy in sends:
        copy.wait_send()


def last_layer(a_ref, h_ref, s_ref, w_ref, oh_ref, os_ref):
    here = pl.ds(pl.program_id(0) * STEP, STEP)
    a = a_ref[here].reshape(STEP * BLOCK, CHAN)
    oh_ref[...] = h_ref[here] + dot(a, w_ref[0]).reshape(oh_ref.shape)
    os_ref[...] = s_ref[here] + dot(a, w_ref[1]).reshape(os_ref.shape)


def solution(mesh):
    act_spec = P('dp', 'sp', None)

    def local_stack(x, w_in, w_res, w_skip):
        vmem = lambda shape, dtype: pltpu.VMEM(shape, dtype)
        dma = lambda *shape: pltpu.SemaphoreType.DMA(shape)
        out = jax.ShapeDtypeStruct((4, 2, BLOCK, CHAN), F32)
        scratch = [vmem((SEQ + 2 * pad_rows(k), CHAN), BF16) for k in range(LAYERS)]
        scratch += [vmem((3, CHIP + 2 * MARGIN[k], CHAN), BF16) for k in range(LOCAL)]
        scratch += [vmem((LAYERS, 3 * CHAN, 2 * CHAN), BF16), vmem((LAYERS * CHAN, CHAN), BF16), vmem((LAYERS * CHAN, CHAN), BF16),
                    vmem((SEQ, CHAN), F32), vmem((3, CHIP + 2 * EDGE, CHAN), F32), vmem((3, CHIP, CHAN), F32), vmem((CHIP, CHAN), F32),
                    vmem((4, 2, BLOCK, CHAN), F32), vmem((4, 2, BLOCK, CHAN), F32),
                    vmem((LAYERS, SEQ, CHAN), BF16), vmem((LAYERS - LOCAL - 1, 8, BLOCK, CHAN), BF16)]
        scratch += [dma(LAYERS, 3), dma(8), dma(8), dma(4), dma(4), dma(4), dma(2, 4, 2), dma(2, 3, 2),
                    dma(LAYERS - LOCAL, 8), dma(LAYERS - LOCAL, 8), dma(4, 2), dma(4, 2), dma(4, 2), dma(4), pltpu.SemaphoreType.REGULAR]
        h, s, a, w = pl.pallas_call(
            kernel,
            out_shape=(out, out, jax.ShapeDtypeStruct((8, BLOCK, CHAN), BF16), jax.ShapeDtypeStruct((2, CHAN, CHAN), BF16)),
            in_specs=[pl.BlockSpec(memory_space=pltpu.HBM)] * 4,
            out_specs=(pl.BlockSpec(memory_space=pl.ANY),) * 4,
            scratch_shapes=scratch,
            compiler_params=pltpu.CompilerParams(collective_id=0, has_side_effects=True, vmem_limit_bytes=VMEM_LIMIT),
        )(pltpu.with_memory_space_constraint(x.reshape(4, 2, BLOCK, CHAN), pltpu.HBM), w_in.reshape(LAYERS, 3 * CHAN, 2 * CHAN), w_res, w_skip)
        rows = pl.BlockSpec((STEP, BLOCK, CHAN), lambda i: (i, 0, 0))
        return pl.pallas_call(
            last_layer,
            grid=(8 // STEP,),
            out_shape=(jax.ShapeDtypeStruct(x.shape, F32),) * 2,
            in_specs=[pl.BlockSpec(memory_space=pltpu.VMEM)] * 4,
            out_specs=(rows, rows),
            compiler_params=pltpu.CompilerParams(vmem_limit_bytes=8 * 2 ** 20),
        )(a, h.reshape(x.shape), s.reshape(x.shape), w)

    return jax.shard_map(local_stack, mesh=mesh, in_specs=(act_spec, P(), P(), P()), out_specs=(act_spec, act_spec), check_vma=False)
```

```python
import functools

import jax
import jax.numpy as jnp
from jax import lax
from jax.experimental import pallas as pl
from jax.experimental.pallas import tpu as pltpu
from jax.sharding import PartitionSpec as P

F32, BF16 = jnp.float32, jnp.bfloat16
MESH = pl.DeviceIdType.MESH
LAYERS = 10
LOCAL = 8
SEQ, BLOCK, CHIP, CHAN = 1024, 128, 256, 256
TILE = 512
INNER = 3
EARLY = 3
STEP = 4
VMEM_LIMIT = 50 * 2 ** 20


HALO = 160
EXTRA = [max(HALO - 2 ** (k + 1) + 15, 0) // 16 * 16 for k in range(LOCAL)]
MARGIN = [EXTRA[k] + max(2 ** k, 16) for k in range(LOCAL)]
EDGE = MARGIN[-1] - EXTRA[-2]


def pad_rows(layer):
    return max(2 ** layer, 16)


def flip(index, q):
    out = index
    for bit in range(3):
        if q >> bit & 1:
            out = out + 2 ** bit - 2 ** (bit + 1) * lax.rem(lax.div(index, 2 ** bit), 2)
    return out


def taps(load, d, n):
    centre = load(0, n)
    if d < 16:
        wide = load(-16, n + 32)
        return jnp.concatenate([wide[16 - d:16 - d + n], centre, wide[16 + d:16 + d + n]], axis=1)
    return jnp.concatenate([load(-d, n), centre, load(d, n)], axis=1)


def gated(z):
    half = jnp.tanh(z[:, CHAN:] * 0.5)
    return (jnp.tanh(z[:, :CHAN]) * (0.5 + 0.5 * half)).astype(BF16)


def dot(a, b):
    return jnp.dot(a, b, preferred_element_type=F32)


def kernel(x_ref, win_hbm, wres_hbm, wskip_hbm, oh_ref, os_ref, a_ref, w_ref, *scratch):
    su = scratch[:LAYERS]
    hu = scratch[LAYERS:LAYERS + LOCAL]
    (win, wres, wskip, hseq, hh, hs, own_s, sa,
     wsem, xsend, xrecv, xloc, psend, precv, hsend, hrecv, asend, arecv, fsend, frecv, floc, osem, relay) = scratch[LAYERS + LOCAL:]

    me = lax.axis_index('sp')
    chip, core = lax.div(me, 2), lax.rem(me, 2)
    partner = flip(me, 1)
    pair = [chip] + [lax.rem(chip + r, 4) for r in (1, 2, 3)]

    def remote(src, dst, send, recv, device):
        return pltpu.make_async_remote_copy(src_ref=src, dst_ref=dst, send_sem=send, recv_sem=recv,
                                            device_id={'sp': device}, device_id_type=MESH)

    def block(start, size=BLOCK):
        return pl.ds(pl.multiple_of(start, 16), size)

    weights = []
    for k in range(LAYERS):
        row = [pltpu.make_async_copy(win_hbm.at[k], win.at[k], wsem.at[k, 0]),
               pltpu.make_async_copy(wres_hbm.at[k], wres.at[pl.ds(k * CHAN, CHAN)], wsem.at[k, 1]),
               pltpu.make_async_copy(wskip_hbm.at[k], wskip.at[pl.ds(k * CHAN, CHAN)], wsem.at[k, 2])]
        for copy in row:
            copy.start()
        weights.append(row)

    barrier = pltpu.get_barrier_semaphore()
    for q in range(1, 6):
        pl.semaphore_signal(barrier, inc=1, device_id={'sp': flip(me, q)}, device_id_type=MESH)
    own_rows = block(16 + BLOCK * me)
    half_rows = block(MARGIN[0] + BLOCK * core)
    local = [pltpu.make_async_copy(x_ref.at[chip, core], su[0].at[own_rows], xloc.at[0])]
    local += [pltpu.make_async_copy(x_ref.at[pair[r], core], hu[0].at[r - 1, half_rows], xloc.at[r]) for r in (1, 2, 3)]
    for copy in local:
        copy.start()
    for k in range(LAYERS):
        pad = pad_rows(k)
        su[k][:pad, :] = jnp.zeros((pad, CHAN), BF16)
        su[k][pad + SEQ:, :] = jnp.zeros((pad, CHAN), BF16)
    for k in range(3):
        assert MARGIN[k] == 16 + (EXTRA[k - 1] if k else HALO)
        for r in range(3):
            hu[k][r, :16, :] = jnp.zeros((16, CHAN), BF16)
            hu[k][r, CHIP + 2 * MARGIN[k] - 16:, :] = jnp.zeros((16, CHAN), BF16)
    pl.semaphore_wait(barrier, 5)
    pl.semaphore_signal(relay, inc=1, device_id={'sp': flip(me, 2)}, device_id_type=MESH)

    spread = {}
    for q in (2, 4, 3, 5, 1, 6, 7):
        if q == 6:
            pl.semaphore_wait(relay, 1)
        to = flip(me, q)
        spread[q] = remote(x_ref.at[lax.div(to, 2), lax.rem(to, 2)], su[0].at[own_rows], xsend.at[q], xrecv.at[q], to)
        spread[q].start()
    mates = [remote(x_ref.at[pair[r], 1 - core], hu[0].at[r - 1, half_rows], psend.at[r], precv.at[r], partner) for r in (1, 2, 3)]
    for copy in mates:
        copy.start()

    sends = []

    def start_if(cond, copy):
        pl.when(cond)(copy.start)
        sends.append((cond, copy))

    parts = [(0, BLOCK), (1, HALO - BLOCK)] if HALO > BLOCK else [(0, BLOCK)]

    def halo(slot, side, part):
        left = MARGIN[0] - (HALO if part else BLOCK)
        right = MARGIN[0] + CHIP + (BLOCK if part else 0)
        return hu[0].at[slot, block(left + side * (right - left), parts[part][1])]

    for part, size in parts:
        side = core if part else 1 - core
        to_chip = chip + 1 - 2 * side
        slot = 2 - 2 * lax.rem(to_chip + 2, 2)
        rows = block((1 - side) * (BLOCK - size), size)
        for p in range(2):
            copy = remote(x_ref.at[jnp.clip(3 - to_chip, 0, 3), p, rows], halo(slot, side, part), hsend.at[0, p, part],
                          hrecv.at[part, slot, side], jnp.clip(2 * to_chip + p, 0, 7))
            start_if(jnp.logical_and(to_chip >= 0, to_chip <= 3), copy)

    def send_halo():
        for n, q in enumerate((2, 4)):
            to = flip(me, q)
            there = lax.div(to, 2)
            slot = 2 * lax.rem(there, 2) if q == 2 else 1
            for side in range(2):
                for part, size in parts:
                    first = CHIP + part * BLOCK if side else -(HALO if part else BLOCK)
                    src = block(jnp.clip(16 + CHIP * there + first, 0, 32 + SEQ - size), size)
                    copy = remote(su[0].at[src], halo(slot, side, part), hsend.at[1 + part, n, side], hrecv.at[part, slot, side], to)
                    start_if(there < 3 if side else there > 0, copy)

    def wait_halo(side):
        for r in range(3):
            for part, _ in parts:
                dst = halo(r, side, part)
                pltpu.make_async_copy(dst, dst, hrecv.at[part, r, side]).wait()

    last = LOCAL - 1

    def edge(slot, side):
        return hu[last].at[slot, pl.ds(side * (CHIP + 2 * MARGIN[last] - EDGE), EDGE)]

    def send_edges():
        for r in (1, 2, 3):
            for side in range(2):
                src = su[last].at[block(CHIP * pair[r] + side * (CHIP + 2 * MARGIN[last] - EDGE), EDGE)]
                copy = remote(src, edge(3 - r, side), hsend.at[3, r, side], hrecv.at[2, 3 - r, side], 2 * pair[r] + core)
                copy.start()
                sends.append((None, copy))

    def wait_edges():
        for r in range(3):
            for side in range(2):
                dst = edge(r, side)
                pltpu.make_async_copy(dst, dst, hrecv.at[2, r, side]).wait()

    def send_gated(k):
        for q in range(8):
            to = flip(me, q)
            src = sa.at[k, block(BLOCK * to)]
            dst = a_ref.at[k - LOCAL, me]
            if q == 0:
                copy = pltpu.make_async_copy(src, dst, arecv.at[k - LOCAL, 0])
            else:
                copy = remote(src, dst, asend.at[k - LOCAL, q], arecv.at[k - LOCAL, q], to)
                sends.append((None, copy))
            copy.start()

    def wait_gated(k):
        for q in range(8):
            dst = a_ref.at[k - LOCAL, flip(me, q)]
            pltpu.make_async_copy(dst, dst, arecv.at[k - LOCAL, q]).wait()

    def seq_layer(k, tiles):
        d, pad = 2 ** k, pad_rows(k)

        def rows_at(start, size):
            return pl.ds(start if isinstance(start, int) else pl.multiple_of(start, 16), size)

        pre = []
        for row, size in tiles:
            rows, weight = taps(lambda start, n: su[k][rows_at(row + pad + start, n), :], d, size), win[k]
            if d == TILE:
                first = 0 if row else CHAN
                rows, weight = rows[:, first:first + 2 * CHAN], win[k, pl.ds(first, 2 * CHAN), :]
            pre.append(dot(rows, weight))
        for (row, size), z in zip(tiles, pre):
            here = rows_at(row, size)
            a = gated(z)
            sa[k, here, :] = a
            if k < LAYERS - 1:
                new = hseq[here, :] + dot(a, wres[pl.ds(k * CHAN, CHAN), :])
                if k < LOCAL:
                    hseq[here, :] = new
                su[k + 1][rows_at(row + pad_rows(k + 1), size), :] = new.astype(BF16)

    moves = []

    def hand_over(r):
        for n, dst in enumerate((oh_ref, os_ref)):
            def half(which):
                if r:
                    return (hh.at[r - 1, block(HALO + BLOCK * which)], hs.at[r - 1, block(BLOCK * which)])[n]
                return (hseq.at[block(CHIP * chip + BLOCK * which)], own_s.at[block(BLOCK * which)])[n]
            pair_of = [remote(half(1 - core), dst.at[pair[r], core], fsend.at[r, n], frecv.at[r, n], partner),
                       pltpu.make_async_copy(half(core), dst.at[pair[r], core], floc.at[r, n])]
            for move in pair_of:
                move.start()
            moves.extend(pair_of)

    def home_layer(k, ranges):
        d, margin = 2 ** k, MARGIN[k]
        weight = pl.ds(k * CHAN, CHAN)
        pre = [dot(jnp.concatenate([taps(lambda start, n: hu[k][r, pl.ds(margin + first + start, n), :], d, size) for first, size in ranges], axis=0), win[k])
               for r in range(3)]
        for r, z in enumerate(pre):
            a = gated(z)
            res = dot(a, wres[weight, :])
            at = 0
            for first, size in ranges:
                here = pl.ds(HALO + first, size)
                new = hh[r, here, :] + res[at:at + size]
                hh[r, here, :] = new
                for low_row, high_row, inside in ((first, 0, chip > 0), (max(first, 0), min(first + size, CHIP), None), (CHIP, first + size, chip < 3)):
                    if low_row < high_row and k < LOCAL - 1:
                        part = new[low_row - first:high_row - first]
                        part = part if inside is None else jnp.where(inside, part, 0.0)
                        hu[k + 1][r, pl.ds(MARGIN[k + 1] + low_row, high_row - low_row), :] = part.astype(BF16)
                at += size
            at = 0
            for first, size in ranges:
                low_row, high_row = max(first, 0), min(first + size, CHIP)
                skip = dot(a[at + low_row - first:at + high_row - first], wskip[weight, :])
                rows = pl.ds(low_row, high_row - low_row)
                hs[r, rows, :] = skip if k == 0 else hs[r, rows, :] + skip
                at += size
            if k == LOCAL - 1:
                hand_over(r + 1)

    for copy in local[1:] + mates:
        copy.wait()
    for r in range(3):
        hh[r, pl.ds(HALO, CHIP), :] = hu[0][r, pl.ds(MARGIN[0], CHIP), :].astype(F32)
    for k in range(INNER):
        for copy in weights[k]:
            copy.wait()
        home_layer(k, [(16 * (k + 1), CHIP - 32 * (k + 1))])
    low = lax.div(chip, 2)
    local[0].wait()
    for q in (1, 2, 3):
        spread[q].wait()
    near, far = (pl.multiple_of(which * TILE, 16) for which in (low, 1 - low))
    hseq[pl.ds(near, TILE), :] = su[0][pl.ds(pl.multiple_of(16 + near, 16), TILE), :].astype(F32)
    for k in range(EARLY):
        if k >= INNER:
            weights[k][0].wait()
            weights[k][1].wait()
        size = TILE - 16 * (k + 1)
        seq_layer(k, [(low * (SEQ - size), size)])
    for q in (4, 5, 6, 7):
        spread[q].wait()
    send_halo()
    hseq[pl.ds(far, TILE), :] = su[0][pl.ds(pl.multiple_of(16 + far, 16), TILE), :].astype(F32)
    for k in range(LAYERS):
        if k < EARLY:
            size = TILE + 16 * (k + 1)
            start, part = (1 - low) * (SEQ - size), 16 * (size // 32)
            seq_layer(k, [(start, part), (start + part, size - part)])
        else:
            if k >= INNER:
                weights[k][0].wait()
                weights[k][1].wait()
            seq_layer(k, [(row, TILE) for row in range(0, SEQ, TILE)])
        if k == LOCAL - 2:
            send_edges()
        if k >= LOCAL:
            send_gated(k)
    for k in range(INNER, LAYERS):
        weights[k][2].wait()
    final = pl.ds(LOCAL * CHAN, (LAYERS - LOCAL) * CHAN)
    outs = [pltpu.make_async_copy(w.at[final], w_ref.at[n], osem.at[n]) for n, w in enumerate((wres, wskip))]
    for out in outs:
        out.start()
    mine = pl.ds(pl.multiple_of(CHIP * chip, CHIP), CHIP)
    own_s[...] = dot(jnp.concatenate([sa[k, mine, :] for k in range(LOCAL)], axis=1), wskip[pl.ds(0, LOCAL * CHAN), :])
    hand_over(0)
    for side, outer in enumerate((chip == 0, chip == 3)):
        @pl.when(outer)
        def _():
            for r in range(3):
                hu[0][r, pl.ds(16 + side * (CHIP + HALO), HALO), :] = jnp.zeros((HALO, CHAN), BF16)

        @pl.when(jnp.logical_not(outer))
        def _():
            wait_halo(side)
    for r in range(3):
        for first in (-HALO, CHIP):
            hh[r, pl.ds(HALO + first, HALO), :] = hu[0][r, pl.ds(MARGIN[0] + first, HALO), :].astype(F32)
    for k in range(LOCAL):
        if k == LOCAL - 1:
            wait_edges()
        if k < INNER:
            done = 16 * (k + 1)
            home_layer(k, [(-EXTRA[k], EXTRA[k] + done), (CHIP - done, done + EXTRA[k])])
        else:
            home_layer(k, [(-EXTRA[k], CHIP + 2 * EXTRA[k])])
    for out in outs:
        out.wait()
    for move in moves:
        move.wait()
    for k in range(LOCAL, LAYERS):
        wait_gated(k)
    for cond, copy in sends:
        if cond is None:
            copy.wait_send()
        else:
            pl.when(cond)(copy.wait_send)


def last_layers(a_ref, h_ref, s_ref, w_ref, oh_ref, os_ref):
    here = pl.ds(pl.program_id(0) * STEP, STEP)
    a = jnp.concatenate([a_ref[n, here].reshape(STEP * BLOCK, CHAN) for n in range(LAYERS - LOCAL)], axis=1)
    oh_ref[...] = h_ref[here] + dot(a, w_ref[0]).reshape(oh_ref.shape)
    os_ref[...] = s_ref[here] + dot(a, w_ref[1]).reshape(os_ref.shape)


def solution(mesh):
    act_spec = P('dp', 'sp', None)

    def local_stack(x, w_in, w_res, w_skip):
        vmem = lambda shape, dtype: pltpu.VMEM(shape, dtype)
        dma = lambda *shape: pltpu.SemaphoreType.DMA(shape)
        out = jax.ShapeDtypeStruct((4, 2, BLOCK, CHAN), F32)
        scratch = [vmem((SEQ + 2 * pad_rows(k), CHAN), BF16) for k in range(LAYERS)]
        scratch += [vmem((3, CHIP + 2 * MARGIN[k], CHAN), BF16) for k in range(LOCAL)]
        scratch += [vmem((LAYERS, 3 * CHAN, 2 * CHAN), BF16), vmem((LAYERS * CHAN, CHAN), BF16), vmem((LAYERS * CHAN, CHAN), BF16),
                    vmem((SEQ, CHAN), F32), vmem((3, CHIP + 2 * HALO, CHAN), F32), vmem((3, CHIP, CHAN), F32), vmem((CHIP, CHAN), F32),
                    vmem((LAYERS, SEQ, CHAN), BF16)]
        scratch += [dma(LAYERS, 3), dma(8), dma(8), dma(4), dma(4), dma(4), dma(4, 4, 2), dma(3, 3, 2),
                    dma(LAYERS - LOCAL, 8), dma(LAYERS - LOCAL, 8), dma(4, 2), dma(4, 2), dma(4, 2), dma(2), pltpu.SemaphoreType.REGULAR]
        h, s, a, w = pl.pallas_call(
            kernel,
            out_shape=(out, out, jax.ShapeDtypeStruct((LAYERS - LOCAL, 8, BLOCK, CHAN), BF16),
                       jax.ShapeDtypeStruct((2, (LAYERS - LOCAL) * CHAN, CHAN), BF16)),
            in_specs=[pl.BlockSpec(memory_space=pltpu.HBM)] * 4,
            out_specs=(pl.BlockSpec(memory_space=pl.ANY),) * 4,
            scratch_shapes=scratch,
            compiler_params=pltpu.CompilerParams(collective_id=0, has_side_effects=True, vmem_limit_bytes=VMEM_LIMIT),
        )(pltpu.with_memory_space_constraint(x.reshape(4, 2, BLOCK, CHAN), pltpu.HBM), w_in.reshape(LAYERS, 3 * CHAN, 2 * CHAN), w_res, w_skip)
        rows = pl.BlockSpec((STEP, BLOCK, CHAN), lambda i: (i, 0, 0))
        return pl.pallas_call(
            last_layers,
            grid=(8 // STEP,),
            out_shape=(jax.ShapeDtypeStruct(x.shape, F32),) * 2,
            in_specs=[pl.BlockSpec(memory_space=pltpu.VMEM)] * 4,
            out_specs=(rows, rows),
            compiler_params=pltpu.CompilerParams(vmem_limit_bytes=8 * 2 ** 20),
        )(a, h.reshape(x.shape), s.reshape(x.shape), w)

    return jax.shard_map(local_stack, mesh=mesh, in_specs=(act_spec, P(), P(), P()), out_specs=(act_spec, act_spec), check_vma=False)
```

```python
import functools

import jax
import jax.numpy as jnp
from jax import lax
from jax.experimental import pallas as pl
from jax.experimental.pallas import tpu as pltpu
from jax.sharding import PartitionSpec as P

F32, BF16 = jnp.float32, jnp.bfloat16
MESH = pl.DeviceIdType.MESH
LAYERS = 10
LOCAL = 8
SEQ, BLOCK, CHIP, CHAN = 1024, 128, 256, 256
TILE = 512
INNER = 3
EARLY = 4
STEP = 1
VMEM_LIMIT = 50 * 2 ** 20


HALO = 160
EXTRA = [max(HALO - 2 ** (k + 1) + 15, 0) // 16 * 16 for k in range(LOCAL)]
MARGIN = [EXTRA[k] + max(2 ** k, 16) for k in range(LOCAL)]
EDGE = MARGIN[-1] - EXTRA[-2]


def pad_rows(layer):
    return max(2 ** layer, 16)


def flip(index, q):
    out = index
    for bit in range(3):
        if q >> bit & 1:
            out = out + 2 ** bit - 2 ** (bit + 1) * lax.rem(lax.div(index, 2 ** bit), 2)
    return out


def taps(load, d, n):
    centre = load(0, n)
    if d < 16:
        wide = load(-16, n + 32)
        return jnp.concatenate([wide[16 - d:16 - d + n], centre, wide[16 + d:16 + d + n]], axis=1)
    return jnp.concatenate([load(-d, n), centre, load(d, n)], axis=1)


def gated(z):
    half = jnp.tanh(z[:, CHAN:] * 0.5)
    return (jnp.tanh(z[:, :CHAN]) * (0.5 + 0.5 * half)).astype(BF16)


def dot(a, b):
    return jnp.dot(a, b, preferred_element_type=F32)


def kernel(x_ref, win_hbm, wres_hbm, wskip_hbm, oh_ref, os_ref, a_ref, w_ref, *scratch):
    su = scratch[:LAYERS]
    hu = scratch[LAYERS:LAYERS + LOCAL]
    (win, wres, wskip, hseq, hh, hs, own_s, sa,
     wsem, xsend, xrecv, xloc, psend, precv, hsend, hrecv, asend, arecv, fsend, frecv, floc, osem, relay) = scratch[LAYERS + LOCAL:]

    me = lax.axis_index('sp')
    chip, core = lax.div(me, 2), lax.rem(me, 2)
    partner = flip(me, 1)
    pair = [chip] + [lax.rem(chip + r, 4) for r in (1, 2, 3)]

    def remote(src, dst, send, recv, device):
        return pltpu.make_async_remote_copy(src_ref=src, dst_ref=dst, send_sem=send, recv_sem=recv,
                                            device_id={'sp': device}, device_id_type=MESH)

    def block(start, size=BLOCK):
        return pl.ds(pl.multiple_of(start, 16), size)

    weights = []
    for k in range(LAYERS):
        row = [pltpu.make_async_copy(win_hbm.at[k], win.at[k], wsem.at[k, 0]),
               pltpu.make_async_copy(wres_hbm.at[k], wres.at[pl.ds(k * CHAN, CHAN)], wsem.at[k, 1]),
               pltpu.make_async_copy(wskip_hbm.at[k], wskip.at[pl.ds(k * CHAN, CHAN)], wsem.at[k, 2])]
        for copy in row:
            copy.start()
        weights.append(row)

    barrier = pltpu.get_barrier_semaphore()
    for q in range(1, 6):
        pl.semaphore_signal(barrier, inc=1, device_id={'sp': flip(me, q)}, device_id_type=MESH)
    own_rows = block(16 + BLOCK * me)
    half_rows = block(MARGIN[0] + BLOCK * core)
    local = [pltpu.make_async_copy(x_ref.at[chip, core], su[0].at[own_rows], xloc.at[0])]
    local += [pltpu.make_async_copy(x_ref.at[pair[r], core], hu[0].at[r - 1, half_rows], xloc.at[r]) for r in (1, 2, 3)]
    for copy in local:
        copy.start()
    for k in range(LAYERS):
        pad = pad_rows(k)
        su[k][:pad, :] = jnp.zeros((pad, CHAN), BF16)
        su[k][pad + SEQ:, :] = jnp.zeros((pad, CHAN), BF16)
    for k in range(3):
        assert MARGIN[k] == 16 + (EXTRA[k - 1] if k else HALO)
        for r in range(3):
            hu[k][r, :16, :] = jnp.zeros((16, CHAN), BF16)
            hu[k][r, CHIP + 2 * MARGIN[k] - 16:, :] = jnp.zeros((16, CHAN), BF16)
    pl.semaphore_wait(barrier, 5)
    pl.semaphore_signal(relay, inc=1, device_id={'sp': flip(me, 2)}, device_id_type=MESH)

    mates = [remote(x_ref.at[pair[r], 1 - core], hu[0].at[r - 1, half_rows], psend.at[r], precv.at[r], partner) for r in (1, 2, 3)]
    for copy in mates:
        copy.start()

    spread = {}
    for q in (2, 4, 3, 5, 1, 6, 7):
        if q == 6:
            pl.semaphore_wait(relay, 1)
        to = flip(me, q)
        spread[q] = remote(x_ref.at[lax.div(to, 2), lax.rem(to, 2)], su[0].at[own_rows], xsend.at[q], xrecv.at[q], to)
        spread[q].start()
    sends = []

    def start_if(cond, copy):
        pl.when(cond)(copy.start)
        sends.append((cond, copy))

    parts = [(0, BLOCK), (1, HALO - BLOCK)] if HALO > BLOCK else [(0, BLOCK)]

    def halo(slot, side, part):
        left = MARGIN[0] - (HALO if part else BLOCK)
        right = MARGIN[0] + CHIP + (BLOCK if part else 0)
        return hu[0].at[slot, block(left + side * (right - left), parts[part][1])]

    for part, size in parts:
        side = core if part else 1 - core
        to_chip = chip + 1 - 2 * side
        slot = 2 - 2 * lax.rem(to_chip + 2, 2)
        rows = block((1 - side) * (BLOCK - size), size)
        for p in range(2):
            copy = remote(x_ref.at[jnp.clip(3 - to_chip, 0, 3), p, rows], halo(slot, side, part), hsend.at[0, p, part],
                          hrecv.at[part, slot, side], jnp.clip(2 * to_chip + p, 0, 7))
            start_if(jnp.logical_and(to_chip >= 0, to_chip <= 3), copy)

    def send_halo():
        for n, q in enumerate((2, 4)):
            to = flip(me, q)
            there = lax.div(to, 2)
            slot = 2 * lax.rem(there, 2) if q == 2 else 1
            for side in range(2):
                for part, size in parts:
                    first = CHIP + part * BLOCK if side else -(HALO if part else BLOCK)
                    src = block(jnp.clip(16 + CHIP * there + first, 0, 32 + SEQ - size), size)
                    copy = remote(su[0].at[src], halo(slot, side, part), hsend.at[1 + part, n, side], hrecv.at[part, slot, side], to)
                    start_if(there < 3 if side else there > 0, copy)

    def wait_halo(side):
        for r in range(3):
            for part, _ in parts:
                dst = halo(r, side, part)
                pltpu.make_async_copy(dst, dst, hrecv.at[part, r, side]).wait()

    last = LOCAL - 1

    def edge(slot, side):
        return hu[last].at[slot, pl.ds(side * (CHIP + 2 * MARGIN[last] - EDGE), EDGE)]

    def send_edges():
        for r in (1, 2, 3):
            for side in range(2):
                src = su[last].at[block(CHIP * pair[r] + side * (CHIP + 2 * MARGIN[last] - EDGE), EDGE)]
                copy = remote(src, edge(3 - r, side), hsend.at[3, r, side], hrecv.at[2, 3 - r, side], 2 * pair[r] + core)
                copy.start()
                sends.append((None, copy))

    def wait_edges():
        for r in range(3):
            for side in range(2):
                dst = edge(r, side)
                pltpu.make_async_copy(dst, dst, hrecv.at[2, r, side]).wait()

    def send_gated(k):
        for q in range(8):
            to = flip(me, q)
            src = sa.at[k, block(BLOCK * to)]
            dst = a_ref.at[k - LOCAL, me]
            if q == 0:
                copy = pltpu.make_async_copy(src, dst, arecv.at[k - LOCAL, 0])
            else:
                copy = remote(src, dst, asend.at[k - LOCAL, q], arecv.at[k - LOCAL, q], to)
                sends.append((None, copy))
            copy.start()

    def wait_gated(k):
        for q in range(8):
            dst = a_ref.at[k - LOCAL, flip(me, q)]
            pltpu.make_async_copy(dst, dst, arecv.at[k - LOCAL, q]).wait()

    def seq_layer(k, tiles):
        d, pad = 2 ** k, pad_rows(k)

        def rows_at(start, size):
            return pl.ds(start if isinstance(start, int) else pl.multiple_of(start, 16), size)

        pre = []
        for row, size in tiles:
            rows, weight = taps(lambda start, n: su[k][rows_at(row + pad + start, n), :], d, size), win[k]
            if d == TILE:
                first = 0 if row else CHAN
                rows, weight = rows[:, first:first + 2 * CHAN], win[k, pl.ds(first, 2 * CHAN), :]
            pre.append(dot(rows, weight))
        for (row, size), z in zip(tiles, pre):
            here = rows_at(row, size)
            a = gated(z)
            sa[k, here, :] = a
            if k < LAYERS - 1:
                new = hseq[here, :] + dot(a, wres[pl.ds(k * CHAN, CHAN), :])
                if k < LOCAL:
                    hseq[here, :] = new
                su[k + 1][rows_at(row + pad_rows(k + 1), size), :] = new.astype(BF16)

    moves = []

    def hand_over(r):
        for n, dst in enumerate((oh_ref, os_ref)):
            def half(which):
                if r:
                    return (hh.at[r - 1, block(HALO + BLOCK * which)], hs.at[r - 1, block(BLOCK * which)])[n]
                return (hseq.at[block(CHIP * chip + BLOCK * which)], own_s.at[block(BLOCK * which)])[n]
            pair_of = [remote(half(1 - core), dst.at[pair[r], core], fsend.at[r, n], frecv.at[r, n], partner),
                       pltpu.make_async_copy(half(core), dst.at[pair[r], core], floc.at[r, n])]
            for move in pair_of:
                move.start()
            moves.extend(pair_of)

    def home_layer(k, ranges):
        d, margin = 2 ** k, MARGIN[k]
        weight = pl.ds(k * CHAN, CHAN)
        pre = [dot(jnp.concatenate([taps(lambda start, n: hu[k][r, pl.ds(margin + first + start, n), :], d, size) for first, size in ranges], axis=0), win[k])
               for r in range(3)]
        for r, z in enumerate(pre):
            a = gated(z)
            res = dot(a, wres[weight, :])
            at = 0
            for first, size in ranges:
                here = pl.ds(HALO + first, size)
                new = hh[r, here, :] + res[at:at + size]
                hh[r, here, :] = new
                for low_row, high_row, inside in ((first, 0, chip > 0), (max(first, 0), min(first + size, CHIP), None), (CHIP, first + size, chip < 3)):
                    if low_row < high_row and k < LOCAL - 1:
                        part = new[low_row - first:high_row - first]
                        part = part if inside is None else jnp.where(inside, part, 0.0)
                        hu[k + 1][r, pl.ds(MARGIN[k + 1] + low_row, high_row - low_row), :] = part.astype(BF16)
                at += size
            at = 0
            for first, size in ranges:
                low_row, high_row = max(first, 0), min(first + size, CHIP)
                skip = dot(a[at + low_row - first:at + high_row - first], wskip[weight, :])
                rows = pl.ds(low_row, high_row - low_row)
                hs[r, rows, :] = skip if k == 0 else hs[r, rows, :] + skip
                at += size
            if k == LOCAL - 1:
                hand_over(r + 1)

    for copy in local[1:] + mates:
        copy.wait()
    for r in range(3):
        hh[r, pl.ds(HALO, CHIP), :] = hu[0][r, pl.ds(MARGIN[0], CHIP), :].astype(F32)
    for k in range(INNER):
        for copy in weights[k]:
            copy.wait()
        home_layer(k, [(16 * (k + 1), CHIP - 32 * (k + 1))])
    low = lax.div(chip, 2)
    local[0].wait()
    for q in (1, 2, 3):
        spread[q].wait()
    near, far = (pl.multiple_of(which * TILE, 16) for which in (low, 1 - low))
    hseq[pl.ds(near, TILE), :] = su[0][pl.ds(pl.multiple_of(16 + near, 16), TILE), :].astype(F32)
    for k in range(EARLY):
        if k >= INNER:
            weights[k][0].wait()
            weights[k][1].wait()
        size = TILE - 16 * (k + 1)
        seq_layer(k, [(low * (SEQ - size), size)])
    for q in (4, 5, 6, 7):
        spread[q].wait()
    send_halo()
    hseq[pl.ds(far, TILE), :] = su[0][pl.ds(pl.multiple_of(16 + far, 16), TILE), :].astype(F32)
    for k in range(LAYERS):
        if k < EARLY:
            size = TILE + 16 * (k + 1)
            start, part = (1 - low) * (SEQ - size), 16 * (size // 32)
            seq_layer(k, [(start, part), (start + part, size - part)])
        else:
            if k >= INNER:
                weights[k][0].wait()
                weights[k][1].wait()
            seq_layer(k, [(row, TILE) for row in range(0, SEQ, TILE)])
        if k == LOCAL - 2:
            send_edges()
        if k >= LOCAL:
            send_gated(k)
    for k in range(INNER, LAYERS):
        weights[k][2].wait()
    final = pl.ds(LOCAL * CHAN, (LAYERS - LOCAL) * CHAN)
    outs = [pltpu.make_async_copy(w.at[final], w_ref.at[n], osem.at[n]) for n, w in enumerate((wres, wskip))]
    for out in outs:
        out.start()
    mine = pl.ds(pl.multiple_of(CHIP * chip, CHIP), CHIP)
    own_s[...] = dot(jnp.concatenate([sa[k, mine, :] for k in range(LOCAL)], axis=1), wskip[pl.ds(0, LOCAL * CHAN), :])
    hand_over(0)
    for side, outer in enumerate((chip == 0, chip == 3)):
        @pl.when(outer)
        def _():
            for r in range(3):
                hu[0][r, pl.ds(16 + side * (CHIP + HALO), HALO), :] = jnp.zeros((HALO, CHAN), BF16)

        @pl.when(jnp.logical_not(outer))
        def _():
            wait_halo(side)
    for r in range(3):
        for first in (-HALO, CHIP):
            hh[r, pl.ds(HALO + first, HALO), :] = hu[0][r, pl.ds(MARGIN[0] + first, HALO), :].astype(F32)
    for k in range(LOCAL):
        if k == LOCAL - 1:
            wait_edges()
        if k < INNER:
            done = 16 * (k + 1)
            home_layer(k, [(-EXTRA[k], EXTRA[k] + done), (CHIP - done, done + EXTRA[k])])
        else:
            home_layer(k, [(-EXTRA[k], CHIP + 2 * EXTRA[k])])
    for out in outs:
        out.wait()
    for move in moves:
        move.wait()
    for k in range(LOCAL, LAYERS):
        wait_gated(k)
    for cond, copy in sends:
        if cond is None:
            copy.wait_send()
        else:
            pl.when(cond)(copy.wait_send)


def last_layers(a_ref, h_ref, s_ref, w_ref, oh_ref, os_ref, h_new, s_new, sem):
    copies = []
    for i in range(0, 8, STEP):
        here = pl.ds(i, STEP)
        a = jnp.concatenate([a_ref[n, here].reshape(STEP * BLOCK, CHAN) for n in range(LAYERS - LOCAL)], axis=1)
        for n, (old, new, out) in enumerate(((h_ref, h_new, oh_ref), (s_ref, s_new, os_ref))):
            new[here] = old[here] + dot(a, w_ref[n]).reshape(STEP, BLOCK, CHAN)
            copies.append(pltpu.make_async_copy(new.at[here], out.at[here], sem.at[n, i]))
            copies[-1].start()
    for copy in copies:
        copy.wait()


def solution(mesh):
    act_spec = P('dp', 'sp', None)

    def local_stack(x, w_in, w_res, w_skip):
        vmem = lambda shape, dtype: pltpu.VMEM(shape, dtype)
        dma = lambda *shape: pltpu.SemaphoreType.DMA(shape)
        out = jax.ShapeDtypeStruct((4, 2, BLOCK, CHAN), F32)
        scratch = [vmem((SEQ + 2 * pad_rows(k), CHAN), BF16) for k in range(LAYERS)]
        scratch += [vmem((3, CHIP + 2 * MARGIN[k], CHAN), BF16) for k in range(LOCAL)]
        scratch += [vmem((LAYERS, 3 * CHAN, 2 * CHAN), BF16), vmem((LAYERS * CHAN, CHAN), BF16), vmem((LAYERS * CHAN, CHAN), BF16),
                    vmem((SEQ, CHAN), F32), vmem((3, CHIP + 2 * HALO, CHAN), F32), vmem((3, CHIP, CHAN), F32), vmem((CHIP, CHAN), F32),
                    vmem((LAYERS, SEQ, CHAN), BF16)]
        scratch += [dma(LAYERS, 3), dma(8), dma(8), dma(4), dma(4), dma(4), dma(4, 4, 2), dma(3, 3, 2),
                    dma(LAYERS - LOCAL, 8), dma(LAYERS - LOCAL, 8), dma(4, 2), dma(4, 2), dma(4, 2), dma(2), pltpu.SemaphoreType.REGULAR]
        h, s, a, w = pl.pallas_call(
            kernel,
            out_shape=(out, out, jax.ShapeDtypeStruct((LAYERS - LOCAL, 8, BLOCK, CHAN), BF16),
                       jax.ShapeDtypeStruct((2, (LAYERS - LOCAL) * CHAN, CHAN), BF16)),
            in_specs=[pl.BlockSpec(memory_space=pltpu.HBM)] * 4,
            out_specs=(pl.BlockSpec(memory_space=pl.ANY),) * 4,
            scratch_shapes=scratch,
            compiler_params=pltpu.CompilerParams(collective_id=0, has_side_effects=True, vmem_limit_bytes=VMEM_LIMIT),
        )(pltpu.with_memory_space_constraint(x.reshape(4, 2, BLOCK, CHAN), pltpu.HBM), w_in.reshape(LAYERS, 3 * CHAN, 2 * CHAN), w_res, w_skip)
        return pl.pallas_call(
            last_layers,
            out_shape=(jax.ShapeDtypeStruct(x.shape, F32),) * 2,
            in_specs=[pl.BlockSpec(memory_space=pltpu.VMEM)] * 4,
            out_specs=(pl.BlockSpec(memory_space=pl.ANY),) * 2,
            scratch_shapes=[vmem(x.shape, F32), vmem(x.shape, F32), dma(2, 8)],
            compiler_params=pltpu.CompilerParams(vmem_limit_bytes=8 * 2 ** 20),
        )(a, h.reshape(x.shape), s.reshape(x.shape), w)

    return jax.shard_map(local_stack, mesh=mesh, in_specs=(act_spec, P(), P(), P()), out_specs=(act_spec, act_spec), check_vma=False)
```

```python
import functools

import jax
import jax.numpy as jnp
from jax import lax
from jax.experimental import pallas as pl
from jax.experimental.pallas import tpu as pltpu
from jax.sharding import PartitionSpec as P

F32, BF16 = jnp.float32, jnp.bfloat16
MESH = pl.DeviceIdType.MESH
LAYERS = 10
LOCAL = 8
SEQ, BLOCK, CHIP, CHAN = 1024, 128, 256, 256
TILE = 512
INNER = 3
EARLY = 4
STEP = 1
VMEM_LIMIT = 50 * 2 ** 20


HALO = 160
EXTRA = [max(HALO - 2 ** (k + 1) + 15, 0) // 16 * 16 for k in range(LOCAL)]
MARGIN = [EXTRA[k] + max(2 ** k, 16) for k in range(LOCAL)]
EDGE = MARGIN[-1] - EXTRA[-2]


def pad_rows(layer):
    return max(2 ** layer, 16)


def flip(index, q):
    out = index
    for bit in range(3):
        if q >> bit & 1:
            out = out + 2 ** bit - 2 ** (bit + 1) * lax.rem(lax.div(index, 2 ** bit), 2)
    return out


def taps(load, d, n):
    centre = load(0, n)
    if d < 16:
        wide = load(-16, n + 32)
        return jnp.concatenate([wide[16 - d:16 - d + n], centre, wide[16 + d:16 + d + n]], axis=1)
    return jnp.concatenate([load(-d, n), centre, load(d, n)], axis=1)


def gated(z):
    half = jnp.tanh(z[:, CHAN:] * 0.5)
    return (jnp.tanh(z[:, :CHAN]) * (0.5 + 0.5 * half)).astype(BF16)


def dot(a, b):
    return jnp.dot(a, b, preferred_element_type=F32)


def kernel(x_ref, win_hbm, wres_hbm, wskip_hbm, oh_ref, os_ref, a_ref, w_ref, *scratch):
    su = scratch[:LAYERS]
    hu = scratch[LAYERS:LAYERS + LOCAL]
    (win, wres, wskip, hseq, hh, hs, own_s, sa,
     wsem, xsend, xrecv, xloc, psend, precv, hsend, hrecv, asend, arecv, fsend, frecv, floc, osem, relay) = scratch[LAYERS + LOCAL:]

    me = lax.axis_index('sp')
    chip, core = lax.div(me, 2), lax.rem(me, 2)
    partner = flip(me, 1)
    pair = [chip] + [lax.rem(chip + r, 4) for r in (1, 2, 3)]

    def remote(src, dst, send, recv, device):
        return pltpu.make_async_remote_copy(src_ref=src, dst_ref=dst, send_sem=send, recv_sem=recv,
                                            device_id={'sp': device}, device_id_type=MESH)

    def block(start, size=BLOCK):
        return pl.ds(pl.multiple_of(start, 16), size)

    weights = []
    for k in range(LAYERS):
        row = [pltpu.make_async_copy(win_hbm.at[k], win.at[k], wsem.at[k, 0]),
               pltpu.make_async_copy(wres_hbm.at[k], wres.at[pl.ds(k * CHAN, CHAN)], wsem.at[k, 1]),
               pltpu.make_async_copy(wskip_hbm.at[k], wskip.at[pl.ds(k * CHAN, CHAN)], wsem.at[k, 2])]
        for copy in row:
            copy.start()
        weights.append(row)

    barrier = pltpu.get_barrier_semaphore()
    for q in range(1, 6):
        pl.semaphore_signal(barrier, inc=1, device_id={'sp': flip(me, q)}, device_id_type=MESH)
    own_rows = block(16 + BLOCK * me)
    half_rows = block(MARGIN[0] + BLOCK * core)
    local = [pltpu.make_async_copy(x_ref.at[chip, core], su[0].at[own_rows], xloc.at[0])]
    local += [pltpu.make_async_copy(x_ref.at[pair[r], core], hu[0].at[r - 1, half_rows], xloc.at[r]) for r in (1, 2, 3)]
    for copy in local:
        copy.start()
    for k in range(LAYERS):
        pad = pad_rows(k)
        su[k][:pad, :] = jnp.zeros((pad, CHAN), BF16)
        su[k][pad + SEQ:, :] = jnp.zeros((pad, CHAN), BF16)
    for k in range(3):
        assert MARGIN[k] == 16 + (EXTRA[k - 1] if k else HALO)
        for r in range(3):
            hu[k][r, :16, :] = jnp.zeros((16, CHAN), BF16)
            hu[k][r, CHIP + 2 * MARGIN[k] - 16:, :] = jnp.zeros((16, CHAN), BF16)
    pl.semaphore_wait(barrier, 5)
    pl.semaphore_signal(relay, inc=1, device_id={'sp': flip(me, 2)}, device_id_type=MESH)

    mates = [remote(x_ref.at[pair[r], 1 - core], hu[0].at[r - 1, half_rows], psend.at[r], precv.at[r], partner) for r in (1, 2, 3)]
    for copy in mates:
        copy.start()

    spread = {}
    for q in (2, 3, 1, 4, 5, 6, 7):
        if q == 6:
            pl.semaphore_wait(relay, 1)
        to = flip(me, q)
        spread[q] = remote(x_ref.at[lax.div(to, 2), lax.rem(to, 2)], su[0].at[own_rows], xsend.at[q], xrecv.at[q], to)
        spread[q].start()
    sends = []

    def start_if(cond, copy):
        pl.when(cond)(copy.start)
        sends.append((cond, copy))

    parts = [(0, BLOCK), (1, HALO - BLOCK)] if HALO > BLOCK else [(0, BLOCK)]

    def halo(slot, side, part):
        left = MARGIN[0] - (HALO if part else BLOCK)
        right = MARGIN[0] + CHIP + (BLOCK if part else 0)
        return hu[0].at[slot, block(left + side * (right - left), parts[part][1])]

    for part, size in parts:
        side = core if part else 1 - core
        to_chip = chip + 1 - 2 * side
        slot = 2 - 2 * lax.rem(to_chip + 2, 2)
        rows = block((1 - side) * (BLOCK - size), size)
        for p in range(2):
            copy = remote(x_ref.at[jnp.clip(3 - to_chip, 0, 3), p, rows], halo(slot, side, part), hsend.at[0, p, part],
                          hrecv.at[part, slot, side], jnp.clip(2 * to_chip + p, 0, 7))
            start_if(jnp.logical_and(to_chip >= 0, to_chip <= 3), copy)

    def send_halo():
        for n, q in enumerate((2, 4)):
            to = flip(me, q)
            there = lax.div(to, 2)
            slot = 2 * lax.rem(there, 2) if q == 2 else 1
            for side in range(2):
                for part, size in parts:
                    first = CHIP + part * BLOCK if side else -(HALO if part else BLOCK)
                    src = block(jnp.clip(16 + CHIP * there + first, 0, 32 + SEQ - size), size)
                    copy = remote(su[0].at[src], halo(slot, side, part), hsend.at[1 + part, n, side], hrecv.at[part, slot, side], to)
                    start_if(there < 3 if side else there > 0, copy)

    def wait_halo(side):
        for r in range(3):
            for part, _ in parts:
                dst = halo(r, side, part)
                pltpu.make_async_copy(dst, dst, hrecv.at[part, r, side]).wait()

    last = LOCAL - 1

    def edge(slot, side):
        return hu[last].at[slot, pl.ds(side * (CHIP + 2 * MARGIN[last] - EDGE), EDGE)]

    def send_edges():
        for r in (1, 2, 3):
            for side in range(2):
                src = su[last].at[block(CHIP * pair[r] + side * (CHIP + 2 * MARGIN[last] - EDGE), EDGE)]
                copy = remote(src, edge(3 - r, side), hsend.at[3, r, side], hrecv.at[2, 3 - r, side], 2 * pair[r] + core)
                copy.start()
                sends.append((None, copy))

    def wait_edges():
        for r in range(3):
            for side in range(2):
                dst = edge(r, side)
                pltpu.make_async_copy(dst, dst, hrecv.at[2, r, side]).wait()

    def send_gated(k):
        for q in range(8):
            to = flip(me, q)
            src = sa.at[k, block(BLOCK * to)]
            dst = a_ref.at[k - LOCAL, me]
            if q == 0:
                copy = pltpu.make_async_copy(src, dst, arecv.at[k - LOCAL, 0])
            else:
                copy = remote(src, dst, asend.at[k - LOCAL, q], arecv.at[k - LOCAL, q], to)
                sends.append((None, copy))
            copy.start()

    def wait_gated(k):
        for q in range(8):
            dst = a_ref.at[k - LOCAL, flip(me, q)]
            pltpu.make_async_copy(dst, dst, arecv.at[k - LOCAL, q]).wait()

    def seq_layer(k, tiles):
        d, pad = 2 ** k, pad_rows(k)

        def rows_at(start, size):
            return pl.ds(start if isinstance(start, int) else pl.multiple_of(start, 16), size)

        pre = []
        for row, size in tiles:
            rows, weight = taps(lambda start, n: su[k][rows_at(row + pad + start, n), :], d, size), win[k]
            if d == TILE:
                first = 0 if row else CHAN
                rows, weight = rows[:, first:first + 2 * CHAN], win[k, pl.ds(first, 2 * CHAN), :]
            pre.append(dot(rows, weight))
        for (row, size), z in zip(tiles, pre):
            here = rows_at(row, size)
            a = gated(z)
            sa[k, here, :] = a
            if k < LAYERS - 1:
                new = hseq[here, :] + dot(a, wres[pl.ds(k * CHAN, CHAN), :])
                if k < LOCAL:
                    hseq[here, :] = new
                su[k + 1][rows_at(row + pad_rows(k + 1), size), :] = new.astype(BF16)

    moves = []

    def hand_over(r):
        for n, dst in enumerate((oh_ref, os_ref)):
            def half(which):
                if r:
                    return (hh.at[r - 1, block(HALO + BLOCK * which)], hs.at[r - 1, block(BLOCK * which)])[n]
                return (hseq.at[block(CHIP * chip + BLOCK * which)], own_s.at[block(BLOCK * which)])[n]
            pair_of = [remote(half(1 - core), dst.at[pair[r], core], fsend.at[r, n], frecv.at[r, n], partner),
                       pltpu.make_async_copy(half(core), dst.at[pair[r], core], floc.at[r, n])]
            for move in pair_of:
                move.start()
            moves.extend(pair_of)

    def home_layer(k, ranges):
        d, margin = 2 ** k, MARGIN[k]
        weight = pl.ds(k * CHAN, CHAN)
        pre = [dot(jnp.concatenate([taps(lambda start, n: hu[k][r, pl.ds(margin + first + start, n), :], d, size) for first, size in ranges], axis=0), win[k])
               for r in range(3)]
        for r, z in enumerate(pre):
            a = gated(z)
            res = dot(a, wres[weight, :])
            at = 0
            for first, size in ranges:
                here = pl.ds(HALO + first, size)
                new = hh[r, here, :] + res[at:at + size]
                hh[r, here, :] = new
                for low_row, high_row, inside in ((first, 0, chip > 0), (max(first, 0), min(first + size, CHIP), None), (CHIP, first + size, chip < 3)):
                    if low_row < high_row and k < LOCAL - 1:
                        part = new[low_row - first:high_row - first]
                        part = part if inside is None else jnp.where(inside, part, 0.0)
                        hu[k + 1][r, pl.ds(MARGIN[k + 1] + low_row, high_row - low_row), :] = part.astype(BF16)
                at += size
            at = 0
            for first, size in ranges:
                low_row, high_row = max(first, 0), min(first + size, CHIP)
                skip = dot(a[at + low_row - first:at + high_row - first], wskip[weight, :])
                rows = pl.ds(low_row, high_row - low_row)
                hs[r, rows, :] = skip if k == 0 else hs[r, rows, :] + skip
                at += size
            if k == LOCAL - 1:
                hand_over(r + 1)

    for copy in local[1:] + mates:
        copy.wait()
    for r in range(3):
        hh[r, pl.ds(HALO, CHIP), :] = hu[0][r, pl.ds(MARGIN[0], CHIP), :].astype(F32)
    for k in range(INNER):
        for copy in weights[k]:
            copy.wait()
        home_layer(k, [(16 * (k + 1), CHIP - 32 * (k + 1))])
    low = lax.div(chip, 2)
    local[0].wait()
    for q in (1, 2, 3):
        spread[q].wait()
    near, far = (pl.multiple_of(which * TILE, 16) for which in (low, 1 - low))
    hseq[pl.ds(near, TILE), :] = su[0][pl.ds(pl.multiple_of(16 + near, 16), TILE), :].astype(F32)
    for k in range(EARLY):
        if k >= INNER:
            weights[k][0].wait()
            weights[k][1].wait()
        size = TILE - 16 * (k + 1)
        seq_layer(k, [(low * (SEQ - size), size)])
    for q in (4, 5, 6, 7):
        spread[q].wait()
    send_halo()
    hseq[pl.ds(far, TILE), :] = su[0][pl.ds(pl.multiple_of(16 + far, 16), TILE), :].astype(F32)
    for k in range(LAYERS):
        if k < EARLY:
            size = TILE + 16 * (k + 1)
            start, part = (1 - low) * (SEQ - size), 16 * (size // 32)
            seq_layer(k, [(start, part), (start + part, size - part)])
        else:
            if k >= INNER:
                weights[k][0].wait()
                weights[k][1].wait()
            seq_layer(k, [(row, TILE) for row in range(0, SEQ, TILE)])
        if k == LOCAL - 2:
            send_edges()
        if k >= LOCAL:
            send_gated(k)
    for k in range(INNER, LAYERS):
        weights[k][2].wait()
    final = pl.ds(LOCAL * CHAN, (LAYERS - LOCAL) * CHAN)
    outs = [pltpu.make_async_copy(w.at[final], w_ref.at[n], osem.at[n]) for n, w in enumerate((wres, wskip))]
    for out in outs:
        out.start()
    mine = pl.ds(pl.multiple_of(CHIP * chip, CHIP), CHIP)
    own_s[...] = dot(jnp.concatenate([sa[k, mine, :] for k in range(LOCAL)], axis=1), wskip[pl.ds(0, LOCAL * CHAN), :])
    hand_over(0)
    for side, outer in enumerate((chip == 0, chip == 3)):
        @pl.when(outer)
        def _():
            for r in range(3):
                hu[0][r, pl.ds(16 + side * (CHIP + HALO), HALO), :] = jnp.zeros((HALO, CHAN), BF16)

        @pl.when(jnp.logical_not(outer))
        def _():
            wait_halo(side)
    for r in range(3):
        for first in (-HALO, CHIP):
            hh[r, pl.ds(HALO + first, HALO), :] = hu[0][r, pl.ds(MARGIN[0] + first, HALO), :].astype(F32)
    for k in range(LOCAL):
        if k == LOCAL - 1:
            wait_edges()
        if k < INNER:
            done = 16 * (k + 1)
            home_layer(k, [(-EXTRA[k], EXTRA[k] + done), (CHIP - done, done + EXTRA[k])])
        else:
            home_layer(k, [(-EXTRA[k], CHIP + 2 * EXTRA[k])])
    for out in outs:
        out.wait()
    for move in moves:
        move.wait()
    for k in range(LOCAL, LAYERS):
        wait_gated(k)
    for cond, copy in sends:
        if cond is None:
            copy.wait_send()
        else:
            pl.when(cond)(copy.wait_send)


def last_layers(a_ref, h_ref, s_ref, w_ref, oh_ref, os_ref, h_new, s_new, sem):
    copies = []
    for i in range(0, 8, STEP):
        here = pl.ds(i, STEP)
        a = jnp.concatenate([a_ref[n, here].reshape(STEP * BLOCK, CHAN) for n in range(LAYERS - LOCAL)], axis=1)
        for n, (old, new, out) in enumerate(((h_ref, h_new, oh_ref), (s_ref, s_new, os_ref))):
            new[here] = old[here] + dot(a, w_ref[n]).reshape(STEP, BLOCK, CHAN)
            copies.append(pltpu.make_async_copy(new.at[here], out.at[here], sem.at[n, i]))
            copies[-1].start()
    for copy in copies:
        copy.wait()


def solution(mesh):
    act_spec = P('dp', 'sp', None)

    def local_stack(x, w_in, w_res, w_skip):
        vmem = lambda shape, dtype: pltpu.VMEM(shape, dtype)
        dma = lambda *shape: pltpu.SemaphoreType.DMA(shape)
        out = jax.ShapeDtypeStruct((4, 2, BLOCK, CHAN), F32)
        scratch = [vmem((SEQ + 2 * pad_rows(k), CHAN), BF16) for k in range(LAYERS)]
        scratch += [vmem((3, CHIP + 2 * MARGIN[k], CHAN), BF16) for k in range(LOCAL)]
        scratch += [vmem((LAYERS, 3 * CHAN, 2 * CHAN), BF16), vmem((LAYERS * CHAN, CHAN), BF16), vmem((LAYERS * CHAN, CHAN), BF16),
                    vmem((SEQ, CHAN), F32), vmem((3, CHIP + 2 * HALO, CHAN), F32), vmem((3, CHIP, CHAN), F32), vmem((CHIP, CHAN), F32),
                    vmem((LAYERS, SEQ, CHAN), BF16)]
        scratch += [dma(LAYERS, 3), dma(8), dma(8), dma(4), dma(4), dma(4), dma(4, 4, 2), dma(3, 3, 2),
                    dma(LAYERS - LOCAL, 8), dma(LAYERS - LOCAL, 8), dma(4, 2), dma(4, 2), dma(4, 2), dma(2), pltpu.SemaphoreType.REGULAR]
        h, s, a, w = pl.pallas_call(
            kernel,
            out_shape=(out, out, jax.ShapeDtypeStruct((LAYERS - LOCAL, 8, BLOCK, CHAN), BF16),
                       jax.ShapeDtypeStruct((2, (LAYERS - LOCAL) * CHAN, CHAN), BF16)),
            in_specs=[pl.BlockSpec(memory_space=pltpu.HBM)] * 4,
            out_specs=(pl.BlockSpec(memory_space=pl.ANY),) * 4,
            scratch_shapes=scratch,
            compiler_params=pltpu.CompilerParams(collective_id=0, has_side_effects=True, vmem_limit_bytes=VMEM_LIMIT),
        )(pltpu.with_memory_space_constraint(x.reshape(4, 2, BLOCK, CHAN), pltpu.HBM), w_in.reshape(LAYERS, 3 * CHAN, 2 * CHAN), w_res, w_skip)
        return pl.pallas_call(
            last_layers,
            out_shape=(jax.ShapeDtypeStruct(x.shape, F32),) * 2,
            in_specs=[pl.BlockSpec(memory_space=pltpu.VMEM)] * 4,
            out_specs=(pl.BlockSpec(memory_space=pl.ANY),) * 2,
            scratch_shapes=[vmem(x.shape, F32), vmem(x.shape, F32), dma(2, 8)],
            compiler_params=pltpu.CompilerParams(vmem_limit_bytes=8 * 2 ** 20),
        )(a, h.reshape(x.shape), s.reshape(x.shape), w)

    return jax.shard_map(local_stack, mesh=mesh, in_specs=(act_spec, P(), P(), P()), out_specs=(act_spec, act_spec), check_vma=False)
```
